32 devices in a mesh: dom: 8 (over z, y), grp: 4 (over x, core).
Axes of the slice: x: 2, y: 2, z: 4, core: 2. Of those that a mesh axis runs over, the one named last changes fastest.
Arguments:
- deflation: bfloat16 [32, 1024, 3, 2, 128], P(('dom', 'grp')), may hold values from -1.5 to 1.5
- inverse: bfloat16 [32, 2, 1024, 1024], P(('dom', 'grp'))
- operator: bfloat16 [32, 2, 1024, 1024], P(('dom', 'grp'))
- neighbours: int32 [32, 6], P(('dom', 'grp')), may hold values from -1 to 31, as said below
- counts: int32 [32, 6], P(('dom', 'grp')), may hold values from 0 to 256, as said below
- margin_rows: int32 [32, 6, 256], P(('dom', 'grp')), may hold values from 0 to 1023, as said below
- owners: int32 [32, 6, 1], P(('dom', 'grp')), may hold values from 0 to 3; in each aligned block of 6 rows (0 to 5, 6 to 11, ..., all dimensions but the last counted through in order) at most 2 rows name the same one
Outputs:
- owned_blocks: float32 [256, 3, 2, 128, 128], P(('dom', 'grp'))
The draws below stay inside these ranges and needn't reach their ends.
Inputs may be any that keep to these rules, and one draw needn't show every extreme that they name: `neighbours`: entry n of a subdomain's list is the subdomain with the same group index whose dom index is d + o_n modulo 8 (o_n = -3, -2, -1, 1, 2, 3), or -1 where that pair shares no rows; the relation is symmetric. `counts`: equal on both sides of a pair, 0 exactly where the list holds -1, and 256 for some pair in every draw. `margin_rows`: distinct within each slot; for k below the pair's count, entry k on one side and entry k on the other side name the same global edge. `owners`: among one subdomain's 6 blocks no group index is named more than 2 times; some subdomain names one exactly 2 times.
All inputs are finite; a program needn't handle non-finite values.
Results may differ from the reference program's by a relative error of at most 0.0048.
Values may be sent and summed in bfloat16 or wider, within the bound.
No kernel may reach another device: no remote copies, remote signals or barrier semaphores. Data moves between devices by JAX's collectives and lax.ppermute only.
A program may use at most 64 MiB of HBM per device.

```python
import math
import jax
import jax.numpy as jnp
import numpy as np
from jax import lax

EDGES = 1024
K = 128
SETS = 3
MARGIN = 256
SLOTS = 6
SUBS = 32
CAP = 2
N_DOM = 8
N_GRP = 4


OFFSETS = (-3, -2, -1, 1, 2, 3)


def dominant_one(single, real_low, real_high, imag_low, imag_high, real_noise, imag_noise):
    keys = jax.random.split(single, 4)
    factor = EDGES ** (-0.5)
    real_off = jax.random.normal(keys[0], (EDGES, EDGES), jnp.float32)
    imag_off = jax.random.normal(keys[1], (EDGES, EDGES), jnp.float32)
    diag_real = jax.random.uniform(keys[2], (EDGES, 1), jnp.float32, real_low, real_high)
    diag_imag = jax.random.uniform(keys[3], (EDGES, 1), jnp.float32, imag_low, imag_high)
    identity = jnp.eye(EDGES, dtype=jnp.float32)
    real_part = diag_real * identity + real_noise * factor * real_off
    imag_part = diag_imag * identity + imag_noise * factor * imag_off
    return jnp.stack([real_part, imag_part], axis=0).astype(jnp.bfloat16)


def draw_inverse(key, part):
    keys = jax.random.split(jax.random.fold_in(key, 101), SUBS)
    return lax.map(lambda single: dominant_one(single, 0.6, 1.4, -0.3, 0.3, 0.5, 0.3), keys)


def draw_operator(key, part):
    keys = jax.random.split(jax.random.fold_in(key, 202), SUBS)
    return lax.map(lambda single: dominant_one(single, 1.0, 2.0, 0.1, 0.5, 0.6, 0.3), keys)


def pair_tables(key):
    base = jax.random.fold_in(key, 7)
    present = jax.random.randint(jax.random.fold_in(base, 1), (N_DOM, N_GRP, 3), 0, 4) > 0
    drawn = jax.random.randint(jax.random.fold_in(base, 2), (N_DOM, N_GRP, 3), 1, MARGIN + 1)
    present = present.at[0, 0, 0].set(True)
    drawn = drawn.at[0, 0, 0].set(MARGIN)
    present = present.at[:, 0, 2].set(True)
    drawn = drawn.at[0, 0, 2].set(MARGIN)
    dom_index = jnp.arange(N_DOM, dtype=jnp.int32)[:, None]
    grp_index = jnp.arange(N_GRP, dtype=jnp.int32)[None, :]
    neighbour_cols = []
    count_cols = []
    for offset in OFFSETS:
        if offset > 0:
            here = present[:, :, offset - 1]
            sized = drawn[:, :, offset - 1]
        else:
            here = jnp.roll(present[:, :, -offset - 1], -offset, axis=0)
            sized = jnp.roll(drawn[:, :, -offset - 1], -offset, axis=0)
        partner = (dom_index + offset) % N_DOM * N_GRP + grp_index
        neighbour_cols.append(jnp.where(here, partner, -1))
        count_cols.append(jnp.where(here, sized, 0))
    listed = jnp.stack(neighbour_cols, axis=-1).reshape(SUBS, SLOTS).astype(jnp.int32)
    shared = jnp.stack(count_cols, axis=-1).reshape(SUBS, SLOTS).astype(jnp.int32)
    return (listed, shared)


def draw_neighbours(key, part):
    return pair_tables(key)[0]


def draw_counts(key, part):
    return pair_tables(key)[1]


def draw_margin_rows(key, part):
    keys = jax.random.split(jax.random.fold_in(key, 3), SUBS * SLOTS)
    picks = jax.vmap(lambda single: jax.random.permutation(single, EDGES)[:MARGIN])(keys)
    return picks.reshape(SUBS, SLOTS, MARGIN).astype(jnp.int32)


def block_levels(key, extent, cuts, low, high):
    def one(position, parts):
        heights = jax.random.uniform(jax.random.fold_in(jax.random.fold_in(key, 6), position), (parts,), jnp.float32, low / len(cuts), high / len(cuts))
        return jnp.repeat(jnp.exp(heights), extent[position] // parts).reshape((-1,) + (1,) * (len(extent) - position - 1))

    factor_of = one(*cuts[0])
    for cut in cuts[1:]:
        factor_of = factor_of * one(*cut)
    return factor_of


def shared_out(stream_key, own, number, rows, amount, top, bound, slope):
    ranking = jax.random.permutation(stream_key, amount)
    heavy_load, usual = load_shares(amount, rows * top, bound, slope, True), load_shares(amount, rows * top, bound, slope, False)
    places = jnp.arange(amount)

    def named(tallies, rotation):
        used = int((tallies > 0).sum())
        fixed = max(1, used // 4)
        shifted = fixed + (places - fixed + rotation * (used - fixed)) % max(1, amount - fixed)
        return jnp.zeros((amount,), jnp.int32).at[ranking[jnp.where(places < fixed, places, shifted)]].set(jnp.asarray(tallies, jnp.int32))

    tallies = jnp.where(number % 4 == 0, named(heavy_load, number // 4), named(usual, number - number // 4 - 1))
    mixed = jax.random.permutation(jax.random.fold_in(own, 3), amount)
    giver, taker = mixed[0:amount // 2 * 2:2], mixed[1:amount // 2 * 2:2]
    margin = jnp.minimum(tallies[giver] - 1, bound - tallies[taker]) // 2
    margin = jnp.where((giver == ranking[0]) | (taker == ranking[0]) | (tallies[taker] == 0), 0, jnp.maximum(margin, 0))
    shifted = jax.random.randint(jax.random.fold_in(own, 4), (amount // 2,), 0, 1 << 20) % (margin + 1)
    tallies = tallies.at[giver].add(-shifted).at[taker].add(shifted)
    members = jnp.searchsorted(jnp.cumsum(tallies), jnp.arange(rows * top), side="right").astype(jnp.int32)
    listing = members.reshape(top, rows).T
    listing = listing[jax.random.permutation(jax.random.fold_in(own, 1), rows)]
    rotation = jax.random.randint(jax.random.fold_in(own, 2), (rows, 1), 0, top)
    return jnp.take_along_axis(listing, (jnp.arange(top)[None, :] + rotation) % top, axis=1)


def load_shares(amount, total, reach, slope, full):
    weights = [(1 << 20) // math.isqrt(grade ** slope) + 1 for grade in range(1, amount + 1)]
    largest = reach if full else min(reach, max(-(-total // amount), total * weights[0] // sum(weights)))
    least = 1 if total - largest >= amount - 1 else 0
    given, surplus = [largest] + [least] * (amount - 1), total - largest - least * (amount - 1)
    while surplus > 0:
        free = [i for i in range(1, amount) if given[i] < largest] or [i for i in range(1, amount) if given[i] < reach]
        mass, left = sum([weights[i] for i in free]), surplus
        for i in free:
            extra = min(reach - given[i], max(1, left * weights[i] // mass), surplus)
            given[i] = given[i] + extra
            surplus = surplus - extra
    return np.array(given)


def bell_draw(stream_key, shape, deviation, bound, cuts=(), kind=jnp.bfloat16):
    loudness = block_levels(stream_key, shape, cuts, -0.22, 0.18) if cuts else 1.0
    values = jax.random.normal(stream_key, shape, jnp.float32) * deviation * loudness
    return jnp.minimum(jnp.maximum(values, -bound), bound).astype(kind)


def setup_inputs(seed: int = 0) -> dict:
    arg_keys = jax.random.split(jax.random.key(seed), 8)
    deflation = bell_draw(arg_keys[0], (SUBS, EDGES, SETS, 2, K), 0.25, 1.5, ((0, 32),))
    inverse = draw_inverse(jax.random.fold_in(arg_keys[7], 71), 0)
    operator = draw_operator(jax.random.fold_in(arg_keys[7], 71), 0)
    neighbours = draw_neighbours(jax.random.fold_in(arg_keys[7], 71), 0)
    counts = draw_counts(jax.random.fold_in(arg_keys[7], 71), 0)
    margin_rows = draw_margin_rows(jax.random.fold_in(arg_keys[7], 71), 0)
    owners_keys = jax.random.split(jax.random.fold_in(arg_keys[6], 1), SUBS * SLOTS // SLOTS)
    owners_turns = jax.random.permutation(jax.random.fold_in(arg_keys[6], 3), SUBS * SLOTS // SLOTS)
    owners = jax.vmap(lambda own, number: shared_out(jax.random.fold_in(arg_keys[6], 2), own, number, SLOTS, N_GRP, 1, CAP, 2))(owners_keys, owners_turns).reshape((SUBS, SLOTS, 1))
    return dict(deflation=deflation, inverse=inverse, operator=operator, neighbours=neighbours, counts=counts, margin_rows=margin_rows, owners=owners)


OFFSETS = (-3, -2, -1, 1, 2, 3)


def complex_apply(matrix, vectors):
    edges = vectors.shape[0]
    flat = vectors.reshape(edges, -1)
    real_part = jnp.dot(matrix[0], flat, preferred_element_type=jnp.float32).reshape(vectors.shape)
    imag_part = jnp.dot(matrix[1], flat, preferred_element_type=jnp.float32).reshape(vectors.shape)
    result_real = real_part[:, :, 0] - imag_part[:, :, 1]
    result_imag = real_part[:, :, 1] + imag_part[:, :, 0]
    return jnp.stack([result_real, result_imag], axis=2).astype(jnp.bfloat16)


def local_image(inputs):
    inverse_one, operator_one, vectors = inputs
    first = complex_apply(inverse_one, vectors)
    second = complex_apply(inverse_one, first)
    return complex_apply(operator_one, second)


def project_one(inputs):
    projector, arrived = inputs
    shape = projector.shape
    left = projector.reshape(shape[0], shape[1], shape[2], 2 * K).astype(jnp.float32)
    right = arrived.reshape(shape[0], shape[1], shape[2], 2 * K).astype(jnp.float32)
    gram = jnp.einsum("nrsk,nrsl->nskl", left, right, precision=lax.Precision.HIGHEST)
    real_part = gram[:, :, :K, :K] - gram[:, :, K:, K:]
    imag_part = gram[:, :, :K, K:] + gram[:, :, K:, :K]
    return jnp.stack([real_part, imag_part], axis=2)


def take_rows(table, index):
    return table[index]


def reference(deflation, inverse, operator, neighbours, counts, margin_rows, owners):
    vectors = deflation
    images = lax.map(local_image, (inverse, operator, vectors))
    picked = jax.vmap(take_rows)(images, margin_rows)
    positions = jnp.arange(MARGIN, dtype=jnp.int32)
    live = (neighbours[:, :, None] >= 0) & (positions[None, None, :] < counts[:, :, None])
    outgoing = jnp.where(live[..., None, None, None], picked, jnp.zeros((), jnp.bfloat16))
    grid = outgoing.reshape(N_DOM, N_GRP, SLOTS, MARGIN, SETS, 2, K)
    incoming = jnp.stack([jnp.roll(grid[:, :, SLOTS - 1 - index], -OFFSETS[index], axis=0) for index in range(SLOTS)], axis=2)
    incoming = incoming.reshape(SUBS, SLOTS, MARGIN, SETS, 2, K)
    projector = jax.vmap(take_rows)(vectors, margin_rows)
    coupling = lax.map(project_one, (projector, incoming))
    targets = owners[:, :, 0]
    same = targets[:, :, None] == targets[:, None, :]
    slot_ids = jnp.arange(SLOTS, dtype=jnp.int32)
    earlier = slot_ids[None, :] < slot_ids[:, None]
    rank = jnp.sum((same & earlier[None]).astype(jnp.int32), axis=2).astype(jnp.int32)
    place = targets * CAP + rank
    holders = jnp.arange(N_GRP * CAP, dtype=jnp.int32)
    selector = (holders[None, :, None] == place[:, None, :]).astype(jnp.float32)
    routed = jnp.einsum("spn,snwxyz->spwxyz", selector, coupling, precision=lax.Precision.HIGHEST)
    routed = routed.reshape(N_DOM, N_GRP, N_GRP, CAP, SETS, 2, K, K).transpose(0, 2, 1, 3, 4, 5, 6, 7)
    return routed.reshape(SUBS * N_GRP * CAP, SETS, 2, K, K)
```

```python
import functools

import jax
import jax.numpy as jnp
from jax import lax
from jax.experimental import pallas as pl
from jax.experimental.pallas import tpu as pltpu
from jax.sharding import PartitionSpec as P

OFFSETS = (-3, -2, -1, 1, 2, 3)
F32 = jnp.float32
BF16 = jnp.bfloat16
VMEM_LIMIT = 60 * 1024 * 1024


def passed_along(value, axis, steps):
    count = lax.axis_size(axis)
    pairs = [(source, (source + steps) % count) for source in range(count)]
    return lax.ppermute(value, axis, pairs)


def partner(index, hop, count):
    if count & (count - 1) == 0:
        return index ^ hop
    return (index + hop) % count


def hop_to(index, target, count):
    if count & (count - 1) == 0:
        return index ^ target
    return lax.rem(target - index + count, count)


def hop_from(index, hop, count):
    if count & (count - 1) == 0:
        return index ^ hop
    return lax.rem(index - hop + count, count)


def fill_selector(rows_ref, counts_ref, neighbours_ref, selector):
    slots, margin = rows_ref.shape
    edges = selector.shape[1]
    positions = lax.broadcasted_iota(jnp.int32, (1, margin), 1)
    lanes = lax.broadcasted_iota(jnp.int32, (margin, edges), 1).astype(F32)
    masked = []
    for slot in range(8):
        if slot < slots:
            live = (positions < counts_ref[0, slot]) & (neighbours_ref[0, slot] >= 0)
            masked.append(jnp.where(live, rows_ref[slot : slot + 1, :], -1).astype(F32))
        else:
            masked.append(jnp.full((1, margin), -1.0, F32))
    columns = jnp.transpose(jnp.concatenate(masked, axis=0))
    for slot in range(slots):
        hit = columns[:, slot : slot + 1] == lanes
        selector[slot * margin : (slot + 1) * margin, :] = jnp.where(hit, 1.0, 0.0).astype(BF16)


def chain_kernel(
    index, width, counts_ref, neighbours_ref, rows_ref, z_ref, inverse_ref, operator_ref, *rest
):
    slots, margin = rows_ref.shape
    outs, scratch = rest[:slots], rest[slots:]
    (z_in, z_wide, inverse, operator, selector, first_a, first_b, second_a, second_b, image, sems) = scratch
    edges = inverse.shape[1]
    sets = z_in.shape[0] // (2 * edges)
    z_copy = pltpu.make_async_copy(z_ref, z_in, sems.at[0])
    inverse_copy = pltpu.make_async_copy(inverse_ref, inverse, sems.at[1])
    operator_copy = pltpu.make_async_copy(operator_ref, operator, sems.at[2])
    z_copy.start()
    inverse_copy.start()
    operator_copy.start()
    z_copy.wait()
    z_wide[...] = z_in[...].astype(F32)
    real = z_wide[pl.ds(2 * index, edges, stride=2 * sets), :]
    imag = z_wide[pl.ds(2 * index + 1, edges, stride=2 * sets), :]
    first_a[:, :width] = real.astype(BF16)
    first_a[:, width:] = imag.astype(BF16)
    first_b[:, :width] = (-imag).astype(BF16)
    first_b[:, width:] = real.astype(BF16)
    fill_selector(rows_ref, counts_ref, neighbours_ref, selector)
    block = 256

    def apply(matrix, a, b, store):
        def step(i, _):
            at = pl.ds(pl.multiple_of(i * block, block), block)
            total = jnp.dot(matrix[0, at, :], a[...], preferred_element_type=F32)
            total += jnp.dot(matrix[1, at, :], b[...], preferred_element_type=F32)
            store(at, total)
            return 0

        lax.fori_loop(0, edges // block, step, 0)

    def keep(a, b):
        def store(at, total):
            a[at, :] = total.astype(BF16)
            b[at, :width] = (-total[:, width:]).astype(BF16)
            b[at, width:] = total[:, :width].astype(BF16)

        return store

    def keep_image(at, total):
        image[at, :] = total.astype(BF16)

    inverse_copy.wait()
    apply(inverse, first_a, first_b, keep(second_a, second_b))
    apply(inverse, second_a, second_b, keep(first_a, first_b))
    operator_copy.wait()
    apply(operator, first_a, first_b, keep_image)
    for slot in range(slots):
        outs[slot][...] = jnp.dot(
            selector[slot * margin : (slot + 1) * margin, :], image[...], preferred_element_type=F32
        ).astype(BF16)


def chain(index, width, counts, neighbours, rows, z, inverse, operator):
    slots, margin = rows.shape
    edges = inverse.shape[1]
    any_space = pl.BlockSpec(memory_space=pl.ANY)
    smem = pl.BlockSpec(memory_space=pltpu.SMEM)
    vmem = pl.BlockSpec(memory_space=pltpu.VMEM)
    flops = 2 * edges * 2 * width * (6 * edges + slots * margin)
    return pl.pallas_call(
        functools.partial(chain_kernel, index, width),
        out_shape=[jax.ShapeDtypeStruct((margin, 2 * width), BF16)] * slots,
        in_specs=[smem, smem, vmem, any_space, any_space, any_space],
        out_specs=[vmem] * slots,
        scratch_shapes=[
            pltpu.VMEM(z.shape, BF16),
            pltpu.VMEM(z.shape, F32),
            pltpu.VMEM(inverse.shape, BF16),
            pltpu.VMEM(operator.shape, BF16),
            pltpu.VMEM((slots * margin, edges), BF16),
        ]
        + [pltpu.VMEM((edges, 2 * width), BF16)] * 5
        + [pltpu.SemaphoreType.DMA((3,))],
        compiler_params=pltpu.CompilerParams(vmem_limit_bytes=VMEM_LIMIT),
        cost_estimate=pl.CostEstimate(flops=flops, bytes_accessed=12 << 20, transcendentals=0),
        name=f"chain{index}",
    )(counts, neighbours, rows, z, inverse, operator)


def project_kernel(width, counts_ref, neighbours_ref, rows_ref, z_ref, *rest):
    slots, margin = rows_ref.shape
    z_wide, selector, vectors = rest[-3:]
    outs = rest[:-3]
    edges = vectors.shape[0]
    z_wide[...] = z_ref[...].astype(F32)
    fill_selector(rows_ref, counts_ref, neighbours_ref, selector)
    for index, out in enumerate(outs):
        for part in range(2):
            vectors[:, part * width : (part + 1) * width] = z_wide[
                pl.ds(2 * index + part, edges, stride=2 * len(outs)), :
            ].astype(BF16)
        for slot in range(slots):
            picked = jnp.dot(
                selector[slot * margin : (slot + 1) * margin, :],
                vectors[...],
                preferred_element_type=F32,
            )
            out[slot] = jnp.transpose(picked).astype(BF16)


def project(sets, width, counts, neighbours, rows, z):
    slots, margin = rows.shape
    edges = z.shape[0] // (2 * sets)
    smem = pl.BlockSpec(memory_space=pltpu.SMEM)
    vmem = pl.BlockSpec(memory_space=pltpu.VMEM)
    flops = 2 * edges * 2 * width * slots * margin * sets
    return pl.pallas_call(
        functools.partial(project_kernel, width),
        out_shape=[jax.ShapeDtypeStruct((slots, 2 * width, margin), BF16)] * sets,
        in_specs=[smem, smem, vmem, vmem],
        out_specs=[vmem] * sets,
        scratch_shapes=[
            pltpu.VMEM(z.shape, F32),
            pltpu.VMEM((slots * margin, edges), BF16),
            pltpu.VMEM((edges, 2 * width), BF16),
        ],
        compiler_params=pltpu.CompilerParams(vmem_limit_bytes=VMEM_LIMIT),
        cost_estimate=pl.CostEstimate(flops=flops, bytes_accessed=4 << 20, transcendentals=0),
        name="project",
    )(counts, neighbours, rows, z)


def gram_kernel(width, hops, capacity, owners_ref, me_ref, projector_ref, *rest):
    slots = projector_ref.shape[0]
    incoming, outs, packed = rest[:slots], rest[slots : slots + hops], rest[-1]
    me = me_ref[0]
    packed[...] = jnp.zeros_like(packed)
    for slot in range(slots):
        gram = jnp.dot(projector_ref[slot], incoming[slot][...], preferred_element_type=F32)
        owner = owners_ref[0, slot]
        rank = jnp.int32(0)
        for other in range(slot):
            rank += (owners_ref[0, other] == owner).astype(jnp.int32)
        place = hop_to(me, owner, hops) * capacity + rank
        packed[place, 0] = (gram[:width, :width] - gram[width:, width:]).astype(BF16)
        packed[place, 1] = (gram[:width, width:] + gram[width:, :width]).astype(BF16)
    for hop in range(hops):
        outs[hop][...] = packed[hop * capacity : (hop + 1) * capacity]


def gram_blocks(index, width, hops, capacity, owners, me, projector, incoming):
    smem = pl.BlockSpec(memory_space=pltpu.SMEM)
    vmem = pl.BlockSpec(memory_space=pltpu.VMEM)
    block = (capacity, 2, width, width)
    slots, _, margin = projector.shape
    return pl.pallas_call(
        functools.partial(gram_kernel, width, hops, capacity),
        out_shape=[jax.ShapeDtypeStruct(block, BF16)] * hops,
        in_specs=[smem, smem] + [vmem] * (1 + len(incoming)),
        out_specs=[vmem] * hops,
        scratch_shapes=[pltpu.VMEM((hops * capacity,) + block[1:], BF16)],
        compiler_params=pltpu.CompilerParams(vmem_limit_bytes=VMEM_LIMIT),
        cost_estimate=pl.CostEstimate(
            flops=2 * slots * margin * 4 * width * width, bytes_accessed=2 << 20, transcendentals=0
        ),
        name=f"gram{index}",
    )(owners, me, projector, *incoming)


def spread(index, sets, width, capacity, me, arrived, held):
    hops = len(arrived)
    smem = pl.BlockSpec(memory_space=pltpu.SMEM)
    vmem = pl.BlockSpec(memory_space=pltpu.VMEM)
    any_space = pl.BlockSpec(memory_space=pl.ANY)
    places = hops * capacity
    extra = [] if held is None else [held]

    def body(me_ref, *rest):
        inputs, (out_ref, wide, sem) = rest[:hops], rest[-3:]
        spread_body(index, capacity, me_ref, inputs, out_ref, wide, sem)

    return pl.pallas_call(
        body,
        out_shape=jax.ShapeDtypeStruct((places, sets, 2, width, width), F32),
        in_specs=[smem] + [vmem] * hops + [any_space] * len(extra),
        out_specs=any_space,
        scratch_shapes=[
            pltpu.VMEM((places, 2, width, width), F32),
            pltpu.SemaphoreType.DMA,
        ],
        input_output_aliases={1 + hops: 0} if extra else {},
        compiler_params=pltpu.CompilerParams(vmem_limit_bytes=VMEM_LIMIT),
        cost_estimate=pl.CostEstimate(flops=1 << 20, bytes_accessed=2 << 20, transcendentals=0),
        name=f"spread{index}",
    )(me, *arrived, *extra)


def spread_body(index, capacity, me_ref, arrived, out_ref, wide, sem):
    hops = len(arrived)
    me = me_ref[0]
    for hop in range(hops):
        source = hop_from(me, hop, hops)
        for place in range(capacity):
            wide[source * capacity + place] = arrived[hop][place].astype(F32)
    copy = pltpu.make_async_copy(wide, out_ref.at[:, index], sem)
    copy.start()
    copy.wait()


def on_device(deflation, inverse, operator, neighbours, counts, margin_rows, owners):
    _, edges, sets, _, width = deflation.shape
    slots = margin_rows.shape[1]
    group_count = lax.axis_size("grp")
    capacity = (slots + group_count - 1) // group_count
    z = deflation.reshape(edges * sets * 2, width)
    rows = margin_rows[0]
    owned = owners.reshape(1, slots)
    me = lax.axis_index("grp").astype(jnp.int32).reshape(1)
    arrived = []
    for index in range(sets):
        outgoing = chain(index, width, counts, neighbours, rows, z, inverse[0], operator[0])
        pieces = [None] * slots
        for slot, offset in enumerate(OFFSETS):
            pieces[slots - 1 - slot] = passed_along(outgoing[slot], "dom", offset)
        arrived.append(pieces)
    projectors = project(sets, width, counts, neighbours, rows, z)
    result = None
    for index in range(sets):
        blocks = gram_blocks(
            index, width, group_count, capacity, owned, me, projectors[index], arrived[index]
        )
        received = [blocks[0]]
        for hop in range(1, group_count):
            pairs = [(s, partner(s, hop, group_count)) for s in range(group_count)]
            received.append(lax.ppermute(blocks[hop], "grp", pairs))
        result = spread(index, sets, width, capacity, me, received, result)
    return result


def solution(mesh):
    placed = (
        P(("dom", "grp"), None, None, None, None),
        P(("dom", "grp"), None, None, None),
        P(("dom", "grp"), None, None, None),
        P(("dom", "grp"), None),
        P(("dom", "grp"), None),
        P(("dom", "grp"), None, None),
        P(("dom", "grp"), None, None),
    )
    return jax.shard_map(
        on_device,
        mesh=mesh,
        in_specs=placed,
        out_specs=P(("dom", "grp"), None, None, None, None),
        check_vma=False,
    )
```

```python
import functools

import jax
import jax.numpy as jnp
from jax import lax
from jax.experimental import pallas as pl
from jax.experimental.pallas import tpu as pltpu
from jax.sharding import PartitionSpec as P


OFFSETS = (-3, -2, -1, 1, 2, 3)
F32 = jnp.float32
BF16 = jnp.bfloat16
CHAIN_VMEM = 16 * 1024 * 1024
SMALL_VMEM = 12 * 1024 * 1024


def passed_along(value, axis, steps):
    count = lax.axis_size(axis)
    pairs = [(source, (source + steps) % count) for source in range(count)]
    return lax.ppermute(value, axis, pairs)


def partner(index, hop, count):
    if count & (count - 1) == 0:
        return index ^ hop
    return (index + hop) % count


def hop_to(index, target, count):
    if count & (count - 1) == 0:
        return index ^ target
    return lax.rem(target - index + count, count)


def hop_from(index, hop, count):
    if count & (count - 1) == 0:
        return index ^ hop
    return lax.rem(index - hop + count, count)


def fill_selector(rows_ref, counts_ref, neighbours_ref, selector):
    slots, _, margin = rows_ref.shape
    edges = selector.shape[1]
    positions = lax.broadcasted_iota(jnp.int32, (1, margin), 1)
    lanes = lax.broadcasted_iota(jnp.int32, (1, edges), 1).astype(F32)
    masked = []
    for slot in range(8):
        if slot < slots:
            live = (positions < counts_ref[0, slot]) & (neighbours_ref[0, slot] >= 0)
            masked.append(jnp.where(live, rows_ref[slot], -1).astype(F32))
        else:
            masked.append(jnp.full((1, margin), -1.0, F32))
    columns = jnp.transpose(jnp.concatenate(masked, axis=0))
    for slot in range(slots):
        hit = columns[:, slot : slot + 1] == lanes
        selector[slot * margin : (slot + 1) * margin, :] = jnp.where(hit, 1.0, 0.0).astype(BF16)


def gather_vectors(z_wide, index, sets, width, a, b):
    edges = a.shape[0]
    real = z_wide[pl.ds(2 * index, edges, stride=2 * sets), :]
    imag = z_wide[pl.ds(2 * index + 1, edges, stride=2 * sets), :]
    a[:, :width] = real.astype(BF16)
    a[:, width:] = imag.astype(BF16)
    b[:, :width] = (-imag).astype(BF16)
    b[:, width:] = real.astype(BF16)


def apply(matrix, waits, width, a, b, to_a, to_b):
    edges = a.shape[0]
    block = edges // 4
    for part in range(4):
        if part in waits:
            waits[part]()
        at = slice(part * block, (part + 1) * block)
        total = jnp.dot(matrix[0, at, :], a[...], preferred_element_type=F32)
        total += jnp.dot(matrix[1, at, :], b[...], preferred_element_type=F32)
        to_a[at, :] = total.astype(BF16)
        if to_b is not None:
            to_b[at, :width] = (-total[:, width:]).astype(BF16)
            to_b[at, width:] = total[:, :width].astype(BF16)


def pick_rows(selector, image, outs):
    margin = outs[0].shape[0]
    for slot, out in enumerate(outs):
        out[...] = jnp.dot(
            selector[slot * margin : (slot + 1) * margin, :], image[...], preferred_element_type=F32
        ).astype(BF16)


def first_chain_kernel(sets, width, *refs):
    counts_ref, neighbours_ref, rows_ref, z_ref, inverse_ref, operator_ref = refs[:6]
    slots = rows_ref.shape[0]
    outs = refs[6 : 6 + slots]
    inverse, operator, selector, z_wide = refs[6 + slots : 10 + slots]
    z_in, first_a, first_b, second_a, second_b, sems = refs[10 + slots :]
    block = inverse.shape[1] // 2
    z_copy = pltpu.make_async_copy(z_ref, z_in, sems.at[0])
    z_copy.start()

    def fetch(source, target, half, sem):
        at = pl.ds(half * block, block)
        return pltpu.make_async_copy(source.at[:, at], target.at[:, at], sem)

    loads = [fetch(inverse_ref, inverse, half, sems.at[1 + half]) for half in range(2)]
    loads += [fetch(operator_ref, operator, half, sems.at[3 + half]) for half in range(2)]
    loads[0].start()
    loads[1].start()
    fill_selector(rows_ref, counts_ref, neighbours_ref, selector)
    z_copy.wait()
    z_wide[...] = z_in[...].astype(F32)
    gather_vectors(z_wide, 0, sets, width, first_a, first_b)

    def begin():
        loads[0].wait()
        loads[2].start()
        loads[3].start()

    apply(inverse, {0: begin, 2: loads[1].wait}, width, first_a, first_b, second_a, second_b)
    apply(inverse, {}, width, second_a, second_b, first_a, first_b)
    apply(operator, {0: loads[2].wait, 2: loads[3].wait}, width, first_a, first_b, second_a, None)
    pick_rows(selector, second_a, outs)


def in_hbm(*values):
    return [pltpu.with_memory_space_constraint(value, pltpu.HBM) for value in values]


def in_vmem(*values):
    return [pltpu.with_memory_space_constraint(value, pltpu.VMEM) for value in values]


def first_chain(sets, width, counts, neighbours, rows, z, inverse, operator):
    slots, _, margin = rows.shape
    edges = inverse.shape[1]
    hbm = pl.BlockSpec(memory_space=pltpu.HBM)
    smem = pl.BlockSpec(memory_space=pltpu.SMEM)
    vmem = pl.BlockSpec(memory_space=pltpu.VMEM)
    flops = 4 * edges * width * (6 * edges + slots * margin)
    outs = [pltpu.VMEM((margin, 2 * width), BF16)] * slots + [
        pltpu.VMEM(inverse.shape, BF16),
        pltpu.VMEM(operator.shape, BF16),
        pltpu.VMEM((slots * margin, edges), BF16),
        pltpu.VMEM(z.shape, F32),
    ]
    results = pl.pallas_call(
        functools.partial(first_chain_kernel, sets, width),
        out_shape=outs,
        in_specs=[smem, smem, vmem, hbm, hbm, hbm],
        out_specs=[vmem] * len(outs),
        scratch_shapes=[pltpu.VMEM(z.shape, BF16)]
        + [pltpu.VMEM((edges, 2 * width), BF16)] * 4
        + [pltpu.SemaphoreType.DMA((5,))],
        compiler_params=pltpu.CompilerParams(vmem_limit_bytes=CHAIN_VMEM),
        cost_estimate=pl.CostEstimate(flops=flops, bytes_accessed=12 << 20, transcendentals=0),
        name="chain0",
    )(*in_hbm(counts, neighbours, rows, z, inverse, operator))
    return results[:slots], results[slots:]


def next_chain_kernel(index, sets, width, inverse, operator, selector, z_wide, *refs):
    outs, (first_a, first_b, second_a, second_b) = refs[:-4], refs[-4:]
    gather_vectors(z_wide, index, sets, width, first_a, first_b)
    apply(inverse, {}, width, first_a, first_b, second_a, second_b)
    apply(inverse, {}, width, second_a, second_b, first_a, first_b)
    apply(operator, {}, width, first_a, first_b, second_a, None)
    pick_rows(selector, second_a, outs)


def next_chain(index, sets, width, slots, held):
    inverse, _, selector, _ = held
    edges = inverse.shape[1]
    margin = selector.shape[0] // slots
    vmem = pl.BlockSpec(memory_space=pltpu.VMEM)
    flops = 4 * edges * width * (6 * edges + slots * margin)
    return pl.pallas_call(
        functools.partial(next_chain_kernel, index, sets, width),
        out_shape=[pltpu.VMEM((margin, 2 * width), BF16)] * slots,
        in_specs=[vmem] * 4,
        out_specs=[vmem] * slots,
        scratch_shapes=[pltpu.VMEM((edges, 2 * width), BF16)] * 4,
        compiler_params=pltpu.CompilerParams(vmem_limit_bytes=SMALL_VMEM),
        cost_estimate=pl.CostEstimate(flops=flops, bytes_accessed=12 << 20, transcendentals=0),
    )(*in_vmem(*held))


def project_kernel(width, selector, z_wide, *refs):
    outs, turned = refs[:-1], refs[-1]
    edges = turned.shape[1]
    slots, _, margin = outs[0].shape
    for index, out in enumerate(outs):
        for part in range(2):
            turned[part * width : (part + 1) * width, :] = jnp.transpose(
                z_wide[pl.ds(2 * index + part, edges, stride=2 * len(outs)), :]
            ).astype(BF16)
        for slot in range(slots):
            out[slot] = lax.dot_general(
                turned[...],
                selector[slot * margin : (slot + 1) * margin, :],
                (((1,), (1,)), ((), ())),
                preferred_element_type=F32,
            ).astype(BF16)


def project(sets, width, slots, held):
    _, _, selector, z_wide = held
    margin, edges = selector.shape[0] // slots, selector.shape[1]
    vmem = pl.BlockSpec(memory_space=pltpu.VMEM)
    return pl.pallas_call(
        functools.partial(project_kernel, width),
        out_shape=[pltpu.VMEM((slots, 2 * width, margin), BF16)] * sets,
        in_specs=[vmem] * 2,
        out_specs=[vmem] * sets,
        scratch_shapes=[pltpu.VMEM((2 * width, edges), BF16)],
        compiler_params=pltpu.CompilerParams(vmem_limit_bytes=SMALL_VMEM),
        cost_estimate=pl.CostEstimate(
            flops=4 * edges * width * slots * margin * sets, bytes_accessed=6 << 20, transcendentals=0
        ),
        name="project",
    )(*in_vmem(selector, z_wide))


def gram_kernel(group, width, hops, capacity, owners_ref, me_ref, *rest):
    projectors, rest = rest[: len(group)], rest[len(group) :]
    slots = projectors[0].shape[0]
    incoming, outs, packed = rest[:slots], rest[slots : slots + hops], rest[-1]
    me = me_ref[0]
    packed[...] = jnp.zeros_like(packed)
    step = 2 * width
    for slot in range(slots):
        owner = owners_ref[0, slot]
        rank = jnp.int32(0)
        for other in range(slot):
            rank += (owners_ref[0, other] == owner).astype(jnp.int32)
        place = hop_to(me, owner, hops) * capacity + rank
        for at in range(len(group)):
            gram = jnp.dot(
                projectors[at][slot],
                incoming[slot][:, at * step : (at + 1) * step],
                preferred_element_type=F32,
            )
            packed[place, at, 0] = (gram[:width, :width] - gram[width:, width:]).astype(BF16)
            packed[place, at, 1] = (gram[:width, width:] + gram[width:, :width]).astype(BF16)
    for hop in range(hops):
        outs[hop][...] = packed[hop * capacity : (hop + 1) * capacity]


def gram_blocks(group, width, hops, capacity, owners, me, projectors, incoming):
    smem = pl.BlockSpec(memory_space=pltpu.SMEM)
    vmem = pl.BlockSpec(memory_space=pltpu.VMEM)
    block = (capacity, len(group), 2, width, width)
    slots, _, margin = projectors[0].shape
    return pl.pallas_call(
        functools.partial(gram_kernel, group, width, hops, capacity),
        out_shape=[jax.ShapeDtypeStruct(block, BF16)] * hops,
        in_specs=[smem, smem] + [vmem] * (len(group) + len(incoming)),
        out_specs=[vmem] * hops,
        scratch_shapes=[pltpu.VMEM((hops * capacity,) + block[1:], BF16)],
        compiler_params=pltpu.CompilerParams(vmem_limit_bytes=SMALL_VMEM),
        cost_estimate=pl.CostEstimate(
            flops=2 * slots * margin * 4 * width * width * len(group),
            bytes_accessed=2 << 20,
            transcendentals=0,
        ),
    )(owners, me, *projectors, *incoming)


def spread(group, sets, width, capacity, me, arrived, held):
    hops = len(arrived)
    smem = pl.BlockSpec(memory_space=pltpu.SMEM)
    vmem = pl.BlockSpec(memory_space=pltpu.VMEM)
    any_space = pl.BlockSpec(memory_space=pl.ANY)
    places = hops * capacity
    extra = [] if held is None else [held]

    def body(me_ref, *rest):
        inputs, (out_ref, wide, sem) = rest[:hops], rest[-3:]
        mine = me_ref[0]
        copies = []
        for hop in range(hops):
            source = hop_from(mine, hop, hops)
            for place in range(capacity):
                wide[source * capacity + place] = inputs[hop][place].astype(F32)
            span = pl.ds(source * capacity, capacity)
            copy = pltpu.make_async_copy(
                wide.at[span],
                out_ref.at[span, group[0] : group[0] + len(group)],
                sem.at[hop],
            )
            copy.start()
            copies.append(copy)
        for copy in copies:
            copy.wait()

    return pl.pallas_call(
        body,
        out_shape=jax.ShapeDtypeStruct((places, sets, 2, width, width), F32),
        in_specs=[smem] + [vmem] * hops + [any_space] * len(extra),
        out_specs=any_space,
        scratch_shapes=[
            pltpu.VMEM((places, len(group), 2, width, width), F32),
            pltpu.SemaphoreType.DMA((hops,)),
        ],
        input_output_aliases={1 + hops: 0} if extra else {},
        compiler_params=pltpu.CompilerParams(vmem_limit_bytes=SMALL_VMEM),
        cost_estimate=pl.CostEstimate(flops=1 << 20, bytes_accessed=2 << 20, transcendentals=0),
    )(me, *arrived, *extra)


def exchanged(outgoing):
    pieces = [None] * len(outgoing)
    for slot, offset in enumerate(OFFSETS):
        pieces[len(outgoing) - 1 - slot] = passed_along(outgoing[slot], "dom", offset)
    return pieces


def on_device(deflation, inverse, operator, neighbours, counts, margin_rows, owners):
    _, edges, sets, _, width = deflation.shape
    _, slots, margin = margin_rows.shape
    group_count = lax.axis_size("grp")
    capacity = (slots + group_count - 1) // group_count
    z = deflation.reshape(edges * sets * 2, width)
    rows = margin_rows.reshape(slots, 1, margin)
    owned = owners.reshape(1, slots)
    me = lax.axis_index("grp").astype(jnp.int32).reshape(1)
    arrived = []
    for index in range(sets):
        if index == 0:
            outgoing, held = first_chain(
                sets, width, counts, neighbours, rows, z, inverse[0], operator[0]
            )
        else:
            outgoing = next_chain(index, sets, width, slots, held)
        arrived.append(exchanged(outgoing))
    projectors = project(sets, width, slots, held)
    received = []
    for index, pieces in enumerate(arrived):
        blocks = gram_blocks(
            (index,), width, group_count, capacity, owned, me, [projectors[index]], pieces
        )
        sent = [blocks[0]]
        for hop in range(1, group_count):
            pairs = [(s, partner(s, hop, group_count)) for s in range(group_count)]
            sent.append(lax.ppermute(blocks[hop], "grp", pairs))
        received.append(sent)
    result = None
    for index in range(sets):
        result = spread((index,), sets, width, capacity, me, received[index], result)
    return result


def solution(mesh):
    placed = (
        P(("dom", "grp"), None, None, None, None),
        P(("dom", "grp"), None, None, None),
        P(("dom", "grp"), None, None, None),
        P(("dom", "grp"), None),
        P(("dom", "grp"), None),
        P(("dom", "grp"), None, None),
        P(("dom", "grp"), None, None),
    )
    return jax.shard_map(
        on_device,
        mesh=mesh,
        in_specs=placed,
        out_specs=P(("dom", "grp"), None, None, None, None),
        check_vma=False,
    )
```

```python
import functools

import jax
import jax.numpy as jnp
from jax import lax
from jax.experimental import pallas as pl
from jax.experimental.pallas import tpu as pltpu
from jax.sharding import PartitionSpec as P


OFFSETS = (-3, -2, -1, 1, 2, 3)
F32 = jnp.float32
BF16 = jnp.bfloat16
CHAIN_VMEM = 16 * 1024 * 1024
SMALL_VMEM = 12 * 1024 * 1024


def exchange_plan(count):
    wanted = sorted(offset % count for offset in OFFSETS)
    masks = [
        mask
        for mask in range(1, count)
        if all(((node ^ mask) - node) % count in wanted for node in range(count))
    ]
    if count & (count - 1) == 0 and len(masks) == len(OFFSETS):
        masks.sort(key=lambda mask: (mask < count // 2, bin(mask).count("1"), -mask))
        return [("xor", mask) for mask in masks]
    return [("shift", offset) for offset in OFFSETS[::-1]]


def exchange_slot(plan, count, me):
    kind, amount = plan
    if kind == "shift":
        return OFFSETS.index(amount)
    step = lax.rem((me ^ amount) - me + count, count)
    slot = jnp.int32(0)
    for index, offset in enumerate(OFFSETS):
        slot += jnp.where(step == offset % count, index, 0)
    return slot


def partner(index, hop, count):
    if count & (count - 1) == 0:
        return index ^ hop
    return (index + hop) % count


def hop_to(index, target, count):
    if count & (count - 1) == 0:
        return index ^ target
    return lax.rem(target - index + count, count)


def hop_from(index, hop, count):
    if count & (count - 1) == 0:
        return index ^ hop
    return lax.rem(index - hop + count, count)


def fill_selector(plans, count, rows_ref, counts_ref, neighbours_ref, selector):
    slots, _, margin = rows_ref.shape
    edges = selector.shape[1]
    me = lax.axis_index("dom")
    positions = lax.broadcasted_iota(jnp.int32, (1, margin), 1)
    lanes = lax.broadcasted_iota(jnp.int32, (1, edges), 1).astype(F32)
    masked = []
    for place in range(8):
        if place < slots:
            slot = exchange_slot(plans[place], count, me)
            live = (positions < counts_ref[0, slot]) & (neighbours_ref[0, slot] >= 0)
            masked.append(jnp.where(live, rows_ref[slot], -1).astype(F32))
        else:
            masked.append(jnp.full((1, margin), -1.0, F32))
    columns = jnp.transpose(jnp.concatenate(masked, axis=0))
    for place in range(slots):
        hit = columns[:, place : place + 1] == lanes
        selector[place * margin : (place + 1) * margin, :] = jnp.where(hit, 1.0, 0.0).astype(BF16)


def gather_vectors(z_wide, index, sets, width, a, b):
    edges = a.shape[0]
    real = z_wide[pl.ds(2 * index, edges, stride=2 * sets), :]
    imag = z_wide[pl.ds(2 * index + 1, edges, stride=2 * sets), :]
    a[:, :width] = real.astype(BF16)
    a[:, width:] = imag.astype(BF16)
    b[:, :width] = (-imag).astype(BF16)
    b[:, width:] = real.astype(BF16)


def apply(matrix, waits, width, a, b, to_a, to_b):
    edges = a.shape[0]
    block = edges // 4
    for part in range(4):
        if part in waits:
            waits[part]()
        at = slice(part * block, (part + 1) * block)
        total = jnp.dot(matrix[0, at, :], a[...], preferred_element_type=F32)
        total += jnp.dot(matrix[1, at, :], b[...], preferred_element_type=F32)
        to_a[at, :] = total.astype(BF16)
        if to_b is not None:
            to_b[at, :width] = (-total[:, width:]).astype(BF16)
            to_b[at, width:] = total[:, :width].astype(BF16)


def pick_rows(selector, image, outs):
    margin = outs[0].shape[0]
    for slot, out in enumerate(outs):
        out[...] = jnp.dot(
            selector[slot * margin : (slot + 1) * margin, :], image[...], preferred_element_type=F32
        ).astype(BF16)


def first_chain_kernel(plans, count, sets, width, *refs):
    counts, neighbours, rows, z_ref, inverse_ref, operator_ref = refs[:6]
    slots = rows.shape[0]
    outs = refs[6 : 6 + slots]
    inverse, operator, selector, z_wide = refs[6 + slots : 10 + slots]
    z_in, first_a, first_b, second_a, second_b, sems = refs[10 + slots :]
    block = inverse.shape[1] // 2

    def fetch(source, target, part, sem):
        at = pl.ds(part * block, block)
        return pltpu.make_async_copy(source.at[:, at], target.at[:, at], sem)

    z_copy = pltpu.make_async_copy(z_ref, z_in, sems.at[0])
    inverse_loads = [fetch(inverse_ref, inverse, part, sems.at[1 + part]) for part in range(2)]
    operator_loads = [fetch(operator_ref, operator, part, sems.at[3 + part]) for part in range(2)]
    for copy in [z_copy] + inverse_loads:
        copy.start()
    fill_selector(plans, count, rows, counts, neighbours, selector)
    z_copy.wait()
    z_wide[...] = z_in[...].astype(F32)
    gather_vectors(z_wide, 0, sets, width, first_a, first_b)

    def begin():
        inverse_loads[0].wait()
        for copy in operator_loads:
            copy.start()

    waits = {2: inverse_loads[1].wait}
    apply(inverse, {0: begin, **waits}, width, first_a, first_b, second_a, second_b)
    apply(inverse, {}, width, second_a, second_b, first_a, first_b)

    def ready():
        operator_loads[0].wait()
        operator_loads[1].wait()

    apply(operator, {0: ready}, width, first_a, first_b, second_a, None)
    pick_rows(selector, second_a, outs)


def in_hbm(*values):
    return [pltpu.with_memory_space_constraint(value, pltpu.HBM) for value in values]


def in_vmem(*values):
    return [pltpu.with_memory_space_constraint(value, pltpu.VMEM) for value in values]


def first_chain(plans, count, sets, width, counts, neighbours, rows, z, inverse, operator):
    slots, _, margin = rows.shape
    edges = inverse.shape[1]
    hbm = pl.BlockSpec(memory_space=pltpu.HBM)
    smem = pl.BlockSpec(memory_space=pltpu.SMEM)
    vmem = pl.BlockSpec(memory_space=pltpu.VMEM)
    flops = 4 * edges * width * (6 * edges + slots * margin)
    outs = [pltpu.VMEM((margin, 2 * width), BF16)] * slots + [
        pltpu.VMEM(inverse.shape, BF16),
        pltpu.VMEM(operator.shape, BF16),
        pltpu.VMEM((slots * margin, edges), BF16),
        pltpu.VMEM(z.shape, F32),
    ]
    results = pl.pallas_call(
        functools.partial(first_chain_kernel, plans, count, sets, width),
        out_shape=outs,
        in_specs=[smem, smem, vmem, hbm, hbm, hbm],
        out_specs=[vmem] * len(outs),
        scratch_shapes=[
            pltpu.VMEM(z.shape, BF16),
        ]
        + [pltpu.VMEM((edges, 2 * width), BF16)] * 4
        + [pltpu.SemaphoreType.DMA((5,))],
        compiler_params=pltpu.CompilerParams(vmem_limit_bytes=CHAIN_VMEM),
        cost_estimate=pl.CostEstimate(flops=flops, bytes_accessed=12 << 20, transcendentals=0),
        name="chain0",
    )(*in_hbm(counts, neighbours, rows, z, inverse, operator))
    return results[:slots], results[slots:]


def next_chain_kernel(index, sets, width, inverse, operator, selector, z_wide, *refs):
    outs, (first_a, first_b, second_a, second_b) = refs[:-4], refs[-4:]
    gather_vectors(z_wide, index, sets, width, first_a, first_b)
    apply(inverse, {}, width, first_a, first_b, second_a, second_b)
    apply(inverse, {}, width, second_a, second_b, first_a, first_b)
    apply(operator, {}, width, first_a, first_b, second_a, None)
    pick_rows(selector, second_a, outs)


def next_chain(index, sets, width, slots, held):
    inverse, _, selector, _ = held
    edges = inverse.shape[1]
    margin = selector.shape[0] // slots
    vmem = pl.BlockSpec(memory_space=pltpu.VMEM)
    flops = 4 * edges * width * (6 * edges + slots * margin)
    return pl.pallas_call(
        functools.partial(next_chain_kernel, index, sets, width),
        out_shape=[pltpu.VMEM((margin, 2 * width), BF16)] * slots,
        in_specs=[vmem] * 4,
        out_specs=[vmem] * slots,
        scratch_shapes=[pltpu.VMEM((edges, 2 * width), BF16)] * 4,
        compiler_params=pltpu.CompilerParams(vmem_limit_bytes=SMALL_VMEM),
        cost_estimate=pl.CostEstimate(flops=flops, bytes_accessed=12 << 20, transcendentals=0),
    )(*in_vmem(*held))


def project_kernel(width, selector, z_wide, *refs):
    outs, turned = refs[:-1], refs[-1]
    edges = turned.shape[1]
    slots, _, margin = outs[0].shape
    for index, out in enumerate(outs):
        for part in range(2):
            turned[part * width : (part + 1) * width, :] = jnp.transpose(
                z_wide[pl.ds(2 * index + part, edges, stride=2 * len(outs)), :]
            ).astype(BF16)
        for slot in range(slots):
            out[slot] = lax.dot_general(
                turned[...],
                selector[slot * margin : (slot + 1) * margin, :],
                (((1,), (1,)), ((), ())),
                preferred_element_type=F32,
            ).astype(BF16)


def project(sets, width, slots, held):
    _, _, selector, z_wide = held
    margin, edges = selector.shape[0] // slots, selector.shape[1]
    vmem = pl.BlockSpec(memory_space=pltpu.VMEM)
    return pl.pallas_call(
        functools.partial(project_kernel, width),
        out_shape=[pltpu.VMEM((slots, 2 * width, margin), BF16)] * sets,
        in_specs=[vmem] * 2,
        out_specs=[vmem] * sets,
        scratch_shapes=[pltpu.VMEM((2 * width, edges), BF16)],
        compiler_params=pltpu.CompilerParams(vmem_limit_bytes=SMALL_VMEM),
        cost_estimate=pl.CostEstimate(
            flops=4 * edges * width * slots * margin * sets, bytes_accessed=6 << 20, transcendentals=0
        ),
        name="project",
    )(*in_vmem(selector, z_wide))


def gram_kernel(plans, count, group, width, hops, capacity, owners_ref, *rest):
    projectors, rest = rest[: len(group)], rest[len(group) :]
    slots = projectors[0].shape[0]
    incoming, outs, packed = rest[:slots], rest[slots : slots + hops], rest[-1]
    me = lax.axis_index("grp")
    here = lax.axis_index("dom")
    packed[...] = jnp.zeros_like(packed)
    step = 2 * width
    for slot in range(slots):
        mine = exchange_slot(plans[slot], count, here)
        owner = owners_ref[0, mine]
        rank = jnp.int32(0)
        for other in range(slots):
            same = (owners_ref[0, other] == owner) & (other < mine)
            rank += same.astype(jnp.int32)
        place = hop_to(me, owner, hops) * capacity + rank
        for at in range(len(group)):
            gram = jnp.dot(
                projectors[at][slot],
                incoming[slot][:, at * step : (at + 1) * step],
                preferred_element_type=F32,
            )
            packed[place, at, 0] = (gram[:width, :width] - gram[width:, width:]).astype(BF16)
            packed[place, at, 1] = (gram[:width, width:] + gram[width:, :width]).astype(BF16)
    for hop in range(hops):
        outs[hop][...] = packed[hop * capacity : (hop + 1) * capacity]


def gram_blocks(plans, count, group, width, hops, capacity, owners, projectors, incoming):
    smem = pl.BlockSpec(memory_space=pltpu.SMEM)
    vmem = pl.BlockSpec(memory_space=pltpu.VMEM)
    block = (capacity, len(group), 2, width, width)
    slots, _, margin = projectors[0].shape
    return pl.pallas_call(
        functools.partial(gram_kernel, plans, count, group, width, hops, capacity),
        out_shape=[jax.ShapeDtypeStruct(block, BF16)] * hops,
        in_specs=[smem] + [vmem] * (len(group) + len(incoming)),
        out_specs=[vmem] * hops,
        scratch_shapes=[pltpu.VMEM((hops * capacity,) + block[1:], BF16)],
        compiler_params=pltpu.CompilerParams(vmem_limit_bytes=SMALL_VMEM),
        cost_estimate=pl.CostEstimate(
            flops=2 * slots * margin * 4 * width * width * len(group),
            bytes_accessed=2 << 20,
            transcendentals=0,
        ),
    )(owners, *projectors, *incoming)


def spread(group, sets, width, capacity, arrived, held):
    hops = len(arrived)
    vmem = pl.BlockSpec(memory_space=pltpu.VMEM)
    any_space = pl.BlockSpec(memory_space=pl.ANY)
    places = hops * capacity
    extra = [] if held is None else [held]

    def body(*rest):
        inputs, (out_ref, wide, sem) = rest[:hops], rest[-3:]
        mine = lax.axis_index("grp")
        copies = []
        for hop in range(hops):
            source = hop_from(mine, hop, hops)
            for place in range(capacity):
                wide[source * capacity + place] = inputs[hop][place].astype(F32)
            span = pl.ds(source * capacity, capacity)
            copy = pltpu.make_async_copy(
                wide.at[span],
                out_ref.at[span, group[0] : group[0] + len(group)],
                sem.at[hop],
            )
            copy.start()
            copies.append(copy)
        for copy in copies:
            copy.wait()

    return pl.pallas_call(
        body,
        out_shape=jax.ShapeDtypeStruct((places, sets, 2, width, width), F32),
        in_specs=[vmem] * hops + [any_space] * len(extra),
        out_specs=any_space,
        scratch_shapes=[
            pltpu.VMEM((places, len(group), 2, width, width), F32),
            pltpu.SemaphoreType.DMA((hops,)),
        ],
        input_output_aliases={hops: 0} if extra else {},
        compiler_params=pltpu.CompilerParams(vmem_limit_bytes=SMALL_VMEM),
        cost_estimate=pl.CostEstimate(flops=1 << 20, bytes_accessed=2 << 20, transcendentals=0),
    )(*arrived, *extra)


def exchanged(plans, count, outgoing):
    pieces = [None] * len(outgoing)
    for place, (kind, amount) in enumerate(plans):
        if kind == "xor":
            pairs, back = [(node, node ^ amount) for node in range(count)], place
        else:
            pairs = [(node, (node + amount) % count) for node in range(count)]
            back = plans.index((kind, -amount))
        pieces[back] = lax.ppermute(outgoing[place], "dom", pairs)
    return pieces


def on_device(deflation, inverse, operator, neighbours, counts, margin_rows, owners):
    _, edges, sets, _, width = deflation.shape
    _, slots, margin = margin_rows.shape
    group_count = lax.axis_size("grp")
    capacity = (slots + group_count - 1) // group_count
    z = deflation.reshape(edges * sets * 2, width)
    rows = margin_rows.reshape(slots, 1, margin)
    owned = owners.reshape(1, slots)
    count = lax.axis_size("dom")
    plans = exchange_plan(count)
    arrived = []
    for index in range(sets):
        if index == 0:
            outgoing, held = first_chain(
                plans, count, sets, width, counts, neighbours, rows, z, inverse[0], operator[0]
            )
        else:
            outgoing = next_chain(index, sets, width, slots, held)
        arrived.append(exchanged(plans, count, outgoing))
    projectors = project(sets, width, slots, held)
    received = []
    for index, pieces in enumerate(arrived):
        blocks = gram_blocks(
            plans, count, (index,), width, group_count, capacity, owned, [projectors[index]], pieces
        )
        sent = [blocks[0]]
        for hop in range(1, group_count):
            pairs = [(s, partner(s, hop, group_count)) for s in range(group_count)]
            sent.append(lax.ppermute(blocks[hop], "grp", pairs))
        received.append(sent)
    result = None
    for index in range(sets):
        result = spread((index,), sets, width, capacity, received[index], result)
    return result


def solution(mesh):
    placed = (
        P(("dom", "grp"), None, None, None, None),
        P(("dom", "grp"), None, None, None),
        P(("dom", "grp"), None, None, None),
        P(("dom", "grp"), None),
        P(("dom", "grp"), None),
        P(("dom", "grp"), None, None),
        P(("dom", "grp"), None, None),
    )
    return jax.shard_map(
        on_device,
        mesh=mesh,
        in_specs=placed,
        out_specs=P(("dom", "grp"), None, None, None, None),
        check_vma=False,
    )
```

```python
import functools

import jax
import jax.numpy as jnp
from jax import lax
from jax.experimental import pallas as pl
from jax.experimental.pallas import tpu as pltpu
from jax.sharding import PartitionSpec as P


OFFSETS = (-3, -2, -1, 1, 2, 3)
F32 = jnp.float32
BF16 = jnp.bfloat16
CHAIN_VMEM = 16 * 1024 * 1024
SMALL_VMEM = 12 * 1024 * 1024


def exchange_plan(count):
    wanted = sorted(offset % count for offset in OFFSETS)
    masks = [
        mask
        for mask in range(1, count)
        if all(((node ^ mask) - node) % count in wanted for node in range(count))
    ]
    if count & (count - 1) == 0 and len(masks) == len(OFFSETS):
        masks.sort(key=lambda mask: (mask < count // 2, bin(mask).count("1"), -mask))
        return [("xor", mask) for mask in masks]
    return [("shift", offset) for offset in OFFSETS[::-1]]


def exchange_slot(plan, count, me):
    kind, amount = plan
    if kind == "shift":
        return OFFSETS.index(amount)
    step = lax.rem((me ^ amount) - me + count, count)
    slot = jnp.int32(0)
    for index, offset in enumerate(OFFSETS):
        slot += jnp.where(step == offset % count, index, 0)
    return slot


def partner(index, hop, count):
    if count & (count - 1) == 0:
        return index ^ hop
    return (index + hop) % count


def hop_to(index, target, count):
    if count & (count - 1) == 0:
        return index ^ target
    return lax.rem(target - index + count, count)


def hop_from(index, hop, count):
    if count & (count - 1) == 0:
        return index ^ hop
    return lax.rem(index - hop + count, count)


def fill_selector(plans, count, rows_ref, counts_ref, neighbours_ref, selector):
    slots, _, margin = rows_ref.shape
    edges = selector.shape[1]
    me = lax.axis_index("dom")
    positions = lax.broadcasted_iota(jnp.int32, (1, margin), 1)
    lanes = lax.broadcasted_iota(jnp.int32, (1, edges), 1).astype(F32)
    masked = []
    for place in range(8):
        if place < slots:
            slot = exchange_slot(plans[place], count, me)
            live = (positions < counts_ref[0, slot]) & (neighbours_ref[0, slot] >= 0)
            masked.append(jnp.where(live, rows_ref[slot], -1).astype(F32))
        else:
            masked.append(jnp.full((1, margin), -1.0, F32))
    columns = jnp.transpose(jnp.concatenate(masked, axis=0))
    for place in range(slots):
        hit = columns[:, place : place + 1] == lanes
        selector[place * margin : (place + 1) * margin, :] = jnp.where(hit, 1.0, 0.0).astype(BF16)


def gather_vectors(z_wide, index, sets, width, a, b):
    edges = a.shape[0]
    real = z_wide[pl.ds(2 * index, edges, stride=2 * sets), :]
    imag = z_wide[pl.ds(2 * index + 1, edges, stride=2 * sets), :]
    a[:, :width] = real.astype(BF16)
    a[:, width:] = imag.astype(BF16)
    b[:, :width] = (-imag).astype(BF16)
    b[:, width:] = real.astype(BF16)


def apply(matrix, waits, width, a, b, to_a, to_b):
    edges = a.shape[0]
    block = edges // 4
    for part in range(4):
        if part in waits:
            waits[part]()
        at = slice(part * block, (part + 1) * block)
        total = jnp.dot(matrix[0, at, :], a[...], preferred_element_type=F32)
        total += jnp.dot(matrix[1, at, :], b[...], preferred_element_type=F32)
        to_a[at, :] = total.astype(BF16)
        if to_b is not None:
            to_b[at, :width] = (-total[:, width:]).astype(BF16)
            to_b[at, width:] = total[:, :width].astype(BF16)


def pick_rows(selector, image, outs):
    margin = outs[0].shape[0]
    for slot, out in enumerate(outs):
        out[...] = jnp.dot(
            selector[slot * margin : (slot + 1) * margin, :], image[...], preferred_element_type=F32
        ).astype(BF16)


def first_chain_kernel(plans, count, sets, width, *refs):
    counts, neighbours, rows, z_ref, inverse_ref, operator_ref = refs[:6]
    slots = rows.shape[0]
    early = slots // 2
    outs = refs[6 : 6 + early]
    inverse, operator, selector, z_wide, image = refs[6 + early : 11 + early]
    z_in, first_a, first_b, second_a, second_b, sems = refs[11 + early :]
    block = inverse.shape[1] // 2

    def fetch(source, target, part, sem):
        at = pl.ds(part * block, block)
        return pltpu.make_async_copy(source.at[:, at], target.at[:, at], sem)

    z_copy = pltpu.make_async_copy(z_ref, z_in, sems.at[0])
    inverse_loads = [fetch(inverse_ref, inverse, part, sems.at[1 + part]) for part in range(2)]
    operator_loads = [fetch(operator_ref, operator, part, sems.at[3 + part]) for part in range(2)]
    for copy in [z_copy] + inverse_loads:
        copy.start()
    fill_selector(plans, count, rows, counts, neighbours, selector)
    z_copy.wait()
    z_wide[...] = z_in[...].astype(F32)
    gather_vectors(z_wide, 0, sets, width, first_a, first_b)

    def begin():
        inverse_loads[0].wait()
        for copy in operator_loads:
            copy.start()

    waits = {2: inverse_loads[1].wait}
    apply(inverse, {0: begin, **waits}, width, first_a, first_b, second_a, second_b)
    apply(inverse, {}, width, second_a, second_b, first_a, first_b)

    def ready():
        operator_loads[0].wait()
        operator_loads[1].wait()

    apply(operator, {0: ready}, width, first_a, first_b, image, None)
    pick_rows(selector, image, outs)


def later_pick(slots, width, held, image):
    _, _, selector, _ = held
    margin = selector.shape[0] // slots
    early = slots // 2
    vmem = pl.BlockSpec(memory_space=pltpu.VMEM)

    def body(selector_ref, image_ref, *outs):
        pick_rows(selector_ref.at[early * margin :], image_ref, outs)

    return pl.pallas_call(
        body,
        out_shape=[pltpu.VMEM((margin, 2 * width), BF16)] * (slots - early),
        in_specs=[vmem] * 2,
        out_specs=[vmem] * (slots - early),
        compiler_params=pltpu.CompilerParams(vmem_limit_bytes=SMALL_VMEM),
        cost_estimate=pl.CostEstimate(
            flops=4 * image.shape[0] * width * slots * margin // 2,
            bytes_accessed=4 << 20,
            transcendentals=0,
        ),
        name="pick0",
    )(*in_vmem(selector, image))


def in_hbm(*values):
    return [pltpu.with_memory_space_constraint(value, pltpu.HBM) for value in values]


def in_vmem(*values):
    return [pltpu.with_memory_space_constraint(value, pltpu.VMEM) for value in values]


def first_chain(plans, count, sets, width, counts, neighbours, rows, z, inverse, operator):
    slots, _, margin = rows.shape
    edges = inverse.shape[1]
    hbm = pl.BlockSpec(memory_space=pltpu.HBM)
    smem = pl.BlockSpec(memory_space=pltpu.SMEM)
    vmem = pl.BlockSpec(memory_space=pltpu.VMEM)
    flops = 4 * edges * width * (6 * edges + slots * margin)
    early = slots // 2
    outs = [pltpu.VMEM((margin, 2 * width), BF16)] * early + [
        pltpu.VMEM(inverse.shape, BF16),
        pltpu.VMEM(operator.shape, BF16),
        pltpu.VMEM((slots * margin, edges), BF16),
        pltpu.VMEM(z.shape, F32),
        pltpu.VMEM((edges, 2 * width), BF16),
    ]
    results = pl.pallas_call(
        functools.partial(first_chain_kernel, plans, count, sets, width),
        out_shape=outs,
        in_specs=[smem, smem, vmem, hbm, hbm, hbm],
        out_specs=[vmem] * len(outs),
        scratch_shapes=[
            pltpu.VMEM(z.shape, BF16),
        ]
        + [pltpu.VMEM((edges, 2 * width), BF16)] * 4
        + [pltpu.SemaphoreType.DMA((5,))],
        compiler_params=pltpu.CompilerParams(vmem_limit_bytes=CHAIN_VMEM),
        cost_estimate=pl.CostEstimate(flops=flops, bytes_accessed=12 << 20, transcendentals=0),
        name="chain0",
    )(*in_hbm(counts, neighbours, rows, z, inverse, operator))
    return results[:early], results[early:-1], results[-1]


def next_chain_kernel(index, sets, width, inverse, operator, selector, z_wide, *refs):
    outs, (first_a, first_b, second_a, second_b) = refs[:-4], refs[-4:]
    gather_vectors(z_wide, index, sets, width, first_a, first_b)
    apply(inverse, {}, width, first_a, first_b, second_a, second_b)
    apply(inverse, {}, width, second_a, second_b, first_a, first_b)
    apply(operator, {}, width, first_a, first_b, second_a, None)
    pick_rows(selector, second_a, outs)


def next_chain(index, sets, width, slots, held):
    inverse, _, selector, _ = held
    edges = inverse.shape[1]
    margin = selector.shape[0] // slots
    vmem = pl.BlockSpec(memory_space=pltpu.VMEM)
    flops = 4 * edges * width * (6 * edges + slots * margin)
    return pl.pallas_call(
        functools.partial(next_chain_kernel, index, sets, width),
        out_shape=[pltpu.VMEM((margin, 2 * width), BF16)] * slots,
        in_specs=[vmem] * 4,
        out_specs=[vmem] * slots,
        scratch_shapes=[pltpu.VMEM((edges, 2 * width), BF16)] * 4,
        compiler_params=pltpu.CompilerParams(vmem_limit_bytes=SMALL_VMEM),
        cost_estimate=pl.CostEstimate(flops=flops, bytes_accessed=12 << 20, transcendentals=0),
    )(*in_vmem(*held))


def project_kernel(width, selector, z_wide, *refs):
    outs, turned = refs[:-1], refs[-1]
    edges = turned.shape[1]
    slots, _, margin = outs[0].shape
    for index, out in enumerate(outs):
        for part in range(2):
            turned[part * width : (part + 1) * width, :] = jnp.transpose(
                z_wide[pl.ds(2 * index + part, edges, stride=2 * len(outs)), :]
            ).astype(BF16)
        for slot in range(slots):
            out[slot] = lax.dot_general(
                turned[...],
                selector[slot * margin : (slot + 1) * margin, :],
                (((1,), (1,)), ((), ())),
                preferred_element_type=F32,
            ).astype(BF16)


def project(sets, width, slots, held):
    _, _, selector, z_wide = held
    margin, edges = selector.shape[0] // slots, selector.shape[1]
    vmem = pl.BlockSpec(memory_space=pltpu.VMEM)
    return pl.pallas_call(
        functools.partial(project_kernel, width),
        out_shape=[pltpu.VMEM((slots, 2 * width, margin), BF16)] * sets,
        in_specs=[vmem] * 2,
        out_specs=[vmem] * sets,
        scratch_shapes=[pltpu.VMEM((2 * width, edges), BF16)],
        compiler_params=pltpu.CompilerParams(vmem_limit_bytes=SMALL_VMEM),
        cost_estimate=pl.CostEstimate(
            flops=4 * edges * width * slots * margin * sets, bytes_accessed=6 << 20, transcendentals=0
        ),
        name="project",
    )(*in_vmem(selector, z_wide))


def gram_kernel(plans, count, group, width, hops, capacity, owners_ref, *rest):
    projectors, rest = rest[: len(group)], rest[len(group) :]
    slots = projectors[0].shape[0]
    incoming, outs, packed = rest[:slots], rest[slots : slots + hops], rest[-1]
    me = lax.axis_index("grp")
    here = lax.axis_index("dom")
    packed[...] = jnp.zeros_like(packed)
    step = 2 * width
    for slot in range(slots):
        mine = exchange_slot(plans[slot], count, here)
        owner = owners_ref[0, mine]
        rank = jnp.int32(0)
        for other in range(slots):
            same = (owners_ref[0, other] == owner) & (other < mine)
            rank += same.astype(jnp.int32)
        place = hop_to(me, owner, hops) * capacity + rank
        for at in range(len(group)):
            gram = jnp.dot(
                projectors[at][slot],
                incoming[slot][:, at * step : (at + 1) * step],
                preferred_element_type=F32,
            )
            packed[place, at, 0] = (gram[:width, :width] - gram[width:, width:]).astype(BF16)
            packed[place, at, 1] = (gram[:width, width:] + gram[width:, :width]).astype(BF16)
    for hop in range(hops):
        outs[hop][...] = packed[hop * capacity : (hop + 1) * capacity]


def gram_blocks(plans, count, group, width, hops, capacity, owners, projectors, incoming):
    smem = pl.BlockSpec(memory_space=pltpu.SMEM)
    vmem = pl.BlockSpec(memory_space=pltpu.VMEM)
    block = (capacity, len(group), 2, width, width)
    slots, _, margin = projectors[0].shape
    return pl.pallas_call(
        functools.partial(gram_kernel, plans, count, group, width, hops, capacity),
        out_shape=[jax.ShapeDtypeStruct(block, BF16)] * hops,
        in_specs=[smem] + [vmem] * (len(group) + len(incoming)),
        out_specs=[vmem] * hops,
        scratch_shapes=[pltpu.VMEM((hops * capacity,) + block[1:], BF16)],
        compiler_params=pltpu.CompilerParams(vmem_limit_bytes=SMALL_VMEM),
        cost_estimate=pl.CostEstimate(
            flops=2 * slots * margin * 4 * width * width * len(group),
            bytes_accessed=2 << 20,
            transcendentals=0,
        ),
    )(owners, *projectors, *incoming)


def spread(group, sets, width, capacity, arrived, held):
    hops = len(arrived)
    vmem = pl.BlockSpec(memory_space=pltpu.VMEM)
    any_space = pl.BlockSpec(memory_space=pl.ANY)
    places = hops * capacity
    extra = [] if held is None else [held]

    def body(*rest):
        inputs, (out_ref, wide, sem) = rest[:hops], rest[-3:]
        mine = lax.axis_index("grp")
        copies = []
        for hop in range(hops):
            source = hop_from(mine, hop, hops)
            for place in range(capacity):
                wide[source * capacity + place] = inputs[hop][place].astype(F32)
            span = pl.ds(source * capacity, capacity)
            copy = pltpu.make_async_copy(
                wide.at[span],
                out_ref.at[span, group[0] : group[0] + len(group)],
                sem.at[hop],
            )
            copy.start()
            copies.append(copy)
        for copy in copies:
            copy.wait()

    return pl.pallas_call(
        body,
        out_shape=jax.ShapeDtypeStruct((places, sets, 2, width, width), F32),
        in_specs=[vmem] * hops + [any_space] * len(extra),
        out_specs=any_space,
        scratch_shapes=[
            pltpu.VMEM((places, len(group), 2, width, width), F32),
            pltpu.SemaphoreType.DMA((hops,)),
        ],
        input_output_aliases={hops: 0} if extra else {},
        compiler_params=pltpu.CompilerParams(vmem_limit_bytes=SMALL_VMEM),
        cost_estimate=pl.CostEstimate(flops=1 << 20, bytes_accessed=2 << 20, transcendentals=0),
    )(*arrived, *extra)


def exchanged(plans, count, outgoing):
    pieces = [None] * len(outgoing)
    for place, (kind, amount) in enumerate(plans):
        if kind == "xor":
            pairs, back = [(node, node ^ amount) for node in range(count)], place
        else:
            pairs = [(node, (node + amount) % count) for node in range(count)]
            back = plans.index((kind, -amount))
        pieces[back] = lax.ppermute(outgoing[place], "dom", pairs)
    return pieces


def on_device(deflation, inverse, operator, neighbours, counts, margin_rows, owners):
    _, edges, sets, _, width = deflation.shape
    _, slots, margin = margin_rows.shape
    group_count = lax.axis_size("grp")
    capacity = (slots + group_count - 1) // group_count
    z = deflation.reshape(edges * sets * 2, width)
    rows = margin_rows.reshape(slots, 1, margin)
    owned = owners.reshape(1, slots)
    count = lax.axis_size("dom")
    plans = exchange_plan(count)
    arrived = []
    for index in range(sets):
        if index == 0:
            outgoing, held, image = first_chain(
                plans, count, sets, width, counts, neighbours, rows, z, inverse[0], operator[0]
            )
        else:
            outgoing = next_chain(index, sets, width, slots, held)
        if index == 0:
            outgoing = list(outgoing) + list(later_pick(slots, width, held, image))
        arrived.append(exchanged(plans, count, outgoing))
    projectors = project(sets, width, slots, held)
    received = []
    for index, pieces in enumerate(arrived):
        blocks = gram_blocks(
            plans, count, (index,), width, group_count, capacity, owned, [projectors[index]], pieces
        )
        sent = [blocks[0]]
        for hop in range(1, group_count):
            pairs = [(s, partner(s, hop, group_count)) for s in range(group_count)]
            sent.append(lax.ppermute(blocks[hop], "grp", pairs))
        received.append(sent)
    result = None
    for index in range(sets):
        result = spread((index,), sets, width, capacity, received[index], result)
    return result


def solution(mesh):
    placed = (
        P(("dom", "grp"), None, None, None, None),
        P(("dom", "grp"), None, None, None),
        P(("dom", "grp"), None, None, None),
        P(("dom", "grp"), None),
        P(("dom", "grp"), None),
        P(("dom", "grp"), None, None),
        P(("dom", "grp"), None, None),
    )
    return jax.shard_map(
        on_device,
        mesh=mesh,
        in_specs=placed,
        out_specs=P(("dom", "grp"), None, None, None, None),
        check_vma=False,
    )
```

```python
import functools

import jax
import jax.numpy as jnp
from jax import lax
from jax.experimental import pallas as pl
from jax.experimental.pallas import tpu as pltpu
from jax.sharding import PartitionSpec as P


OFFSETS = (-3, -2, -1, 1, 2, 3)
F32 = jnp.float32
BF16 = jnp.bfloat16
CHAIN_VMEM = 16 * 1024 * 1024
SMALL_VMEM = 12 * 1024 * 1024


def exchange_plan(count):
    wanted = sorted(offset % count for offset in OFFSETS)
    masks = [
        mask
        for mask in range(1, count)
        if all(((node ^ mask) - node) % count in wanted for node in range(count))
    ]
    if count & (count - 1) == 0 and len(masks) == len(OFFSETS):
        masks.sort(key=lambda mask: (mask < count // 2, bin(mask).count("1"), -mask))
        return [("xor", mask) for mask in masks]
    return [("shift", offset) for offset in OFFSETS[::-1]]


def exchange_slot(plan, count, me):
    kind, amount = plan
    if kind == "shift":
        return OFFSETS.index(amount)
    step = lax.rem((me ^ amount) - me + count, count)
    slot = jnp.int32(0)
    for index, offset in enumerate(OFFSETS):
        slot += jnp.where(step == offset % count, index, 0)
    return slot


def partner(index, hop, count):
    if count & (count - 1) == 0:
        return index ^ hop
    return (index + hop) % count


def hop_to(index, target, count):
    if count & (count - 1) == 0:
        return index ^ target
    return lax.rem(target - index + count, count)


def hop_from(index, hop, count):
    if count & (count - 1) == 0:
        return index ^ hop
    return lax.rem(index - hop + count, count)


def fill_selector(plans, count, rows_ref, counts_ref, neighbours_ref, selector):
    slots, _, margin = rows_ref.shape
    edges = selector.shape[1]
    me = lax.axis_index("dom")
    positions = lax.broadcasted_iota(jnp.int32, (1, margin), 1)
    lanes = lax.broadcasted_iota(jnp.int32, (1, edges), 1).astype(F32)
    masked = []
    for place in range(8):
        if place < slots:
            slot = exchange_slot(plans[place], count, me)
            live = (positions < counts_ref[0, slot]) & (neighbours_ref[0, slot] >= 0)
            masked.append(jnp.where(live, rows_ref[slot], -1).astype(F32))
        else:
            masked.append(jnp.full((1, margin), -1.0, F32))
    columns = jnp.transpose(jnp.concatenate(masked, axis=0))
    for place in range(slots):
        hit = columns[:, place : place + 1] == lanes
        selector[place * margin : (place + 1) * margin, :] = jnp.where(hit, 1.0, 0.0).astype(BF16)


def gather_vectors(z_wide, index, sets, width, a, b):
    edges = a.shape[0]
    real = z_wide[pl.ds(2 * index, edges, stride=2 * sets), :]
    imag = z_wide[pl.ds(2 * index + 1, edges, stride=2 * sets), :]
    a[:, :width] = real.astype(BF16)
    a[:, width:] = imag.astype(BF16)
    b[:, :width] = (-imag).astype(BF16)
    b[:, width:] = real.astype(BF16)


def apply(matrix, waits, width, a, b, to_a, to_b):
    edges = a.shape[0]
    block = edges // 4
    for part in range(4):
        if part in waits:
            waits[part]()
        at = slice(part * block, (part + 1) * block)
        total = jnp.dot(matrix[0, at, :], a[...], preferred_element_type=F32)
        total += jnp.dot(matrix[1, at, :], b[...], preferred_element_type=F32)
        to_a[at, :] = total.astype(BF16)
        if to_b is not None:
            to_b[at, :width] = (-total[:, width:]).astype(BF16)
            to_b[at, width:] = total[:, :width].astype(BF16)


def pick_rows(selector, image, outs):
    margin = outs[0].shape[0]
    for slot, out in enumerate(outs):
        out[...] = jnp.dot(
            selector[slot * margin : (slot + 1) * margin, :], image[...], preferred_element_type=F32
        ).astype(BF16)


def first_chain_kernel(plans, count, sets, width, *refs):
    z_ref, inverse_ref, operator_ref = refs[3:6]
    slots = refs[2].shape[0]
    early = slots // 2
    outs = refs[6 : 6 + early]
    inverse, operator, selector, z_wide, image = refs[6 + early : 11 + early]
    counts, neighbours, rows, z_in, first_a, first_b, second_a, second_b, sems = refs[11 + early :]
    block = inverse.shape[1] // 2

    def fetch(source, target, part, sem):
        at = pl.ds(part * block, block)
        return pltpu.make_async_copy(source.at[:, at], target.at[:, at], sem)

    z_copy = pltpu.make_async_copy(z_ref, z_in, sems.at[0])
    inverse_loads = [fetch(inverse_ref, inverse, part, sems.at[1 + part]) for part in range(2)]
    operator_loads = [fetch(operator_ref, operator, part, sems.at[3 + part]) for part in range(2)]
    small = [
        pltpu.make_async_copy(source, target, sems.at[5 + index])
        for index, (source, target) in enumerate(zip(refs[:3], (counts, neighbours, rows)))
    ]
    for copy in small + [z_copy] + inverse_loads:
        copy.start()
    for copy in small:
        copy.wait()
    fill_selector(plans, count, rows, counts, neighbours, selector)
    z_copy.wait()
    z_wide[...] = z_in[...].astype(F32)
    gather_vectors(z_wide, 0, sets, width, first_a, first_b)

    def begin():
        inverse_loads[0].wait()
        for copy in operator_loads:
            copy.start()

    waits = {2: inverse_loads[1].wait}
    apply(inverse, {0: begin, **waits}, width, first_a, first_b, second_a, second_b)
    apply(inverse, {}, width, second_a, second_b, first_a, first_b)

    def ready():
        operator_loads[0].wait()
        operator_loads[1].wait()

    apply(operator, {0: ready}, width, first_a, first_b, image, None)
    pick_rows(selector, image, outs)


def later_pick(slots, width, held, image):
    _, _, selector, _ = held
    margin = selector.shape[0] // slots
    early = slots // 2
    vmem = pl.BlockSpec(memory_space=pltpu.VMEM)

    def body(selector_ref, image_ref, *outs):
        pick_rows(selector_ref.at[early * margin :], image_ref, outs)

    return pl.pallas_call(
        body,
        out_shape=[pltpu.VMEM((margin, 2 * width), BF16)] * (slots - early),
        in_specs=[vmem] * 2,
        out_specs=[vmem] * (slots - early),
        compiler_params=pltpu.CompilerParams(vmem_limit_bytes=SMALL_VMEM),
        cost_estimate=pl.CostEstimate(
            flops=4 * image.shape[0] * width * slots * margin // 2,
            bytes_accessed=4 << 20,
            transcendentals=0,
        ),
        name="pick0",
    )(*in_vmem(selector, image))


def in_hbm(*values):
    return [pltpu.with_memory_space_constraint(value, pltpu.HBM) for value in values]


def in_vmem(*values):
    return [pltpu.with_memory_space_constraint(value, pltpu.VMEM) for value in values]


def first_chain(plans, count, sets, width, counts, neighbours, rows, z, inverse, operator):
    slots, _, margin = rows.shape
    edges = inverse.shape[1]
    hbm = pl.BlockSpec(memory_space=pltpu.HBM)
    vmem = pl.BlockSpec(memory_space=pltpu.VMEM)
    flops = 4 * edges * width * (6 * edges + slots * margin)
    early = slots // 2
    outs = [pltpu.VMEM((margin, 2 * width), BF16)] * early + [
        pltpu.VMEM(inverse.shape, BF16),
        pltpu.VMEM(operator.shape, BF16),
        pltpu.VMEM((slots * margin, edges), BF16),
        pltpu.VMEM(z.shape, F32),
        pltpu.VMEM((edges, 2 * width), BF16),
    ]
    results = pl.pallas_call(
        functools.partial(first_chain_kernel, plans, count, sets, width),
        out_shape=outs,
        in_specs=[hbm] * 6,
        out_specs=[vmem] * len(outs),
        scratch_shapes=[
            pltpu.SMEM(counts.shape, jnp.int32),
            pltpu.SMEM(neighbours.shape, jnp.int32),
            pltpu.VMEM(rows.shape, jnp.int32),
            pltpu.VMEM(z.shape, BF16),
        ]
        + [pltpu.VMEM((edges, 2 * width), BF16)] * 4
        + [pltpu.SemaphoreType.DMA((8,))],
        compiler_params=pltpu.CompilerParams(vmem_limit_bytes=CHAIN_VMEM),
        cost_estimate=pl.CostEstimate(flops=flops, bytes_accessed=12 << 20, transcendentals=0),
        name="chain0",
    )(*in_hbm(counts, neighbours, rows, z, inverse, operator))
    return results[:early], results[early:-1], results[-1]


def next_chain_kernel(index, sets, width, inverse, operator, selector, z_wide, *refs):
    outs, (first_a, first_b, second_a, second_b) = refs[:-4], refs[-4:]
    gather_vectors(z_wide, index, sets, width, first_a, first_b)
    apply(inverse, {}, width, first_a, first_b, second_a, second_b)
    apply(inverse, {}, width, second_a, second_b, first_a, first_b)
    apply(operator, {}, width, first_a, first_b, second_a, None)
    pick_rows(selector, second_a, outs)


def next_chain(index, sets, width, slots, held):
    inverse, _, selector, _ = held
    edges = inverse.shape[1]
    margin = selector.shape[0] // slots
    vmem = pl.BlockSpec(memory_space=pltpu.VMEM)
    flops = 4 * edges * width * (6 * edges + slots * margin)
    return pl.pallas_call(
        functools.partial(next_chain_kernel, index, sets, width),
        out_shape=[pltpu.VMEM((margin, 2 * width), BF16)] * slots,
        in_specs=[vmem] * 4,
        out_specs=[vmem] * slots,
        scratch_shapes=[pltpu.VMEM((edges, 2 * width), BF16)] * 4,
        compiler_params=pltpu.CompilerParams(vmem_limit_bytes=SMALL_VMEM),
        cost_estimate=pl.CostEstimate(flops=flops, bytes_accessed=12 << 20, transcendentals=0),
    )(*in_vmem(*held))


def project_kernel(width, selector, z_wide, *refs):
    outs, turned = refs[:-1], refs[-1]
    edges = turned.shape[1]
    slots, _, margin = outs[0].shape
    for index, out in enumerate(outs):
        for part in range(2):
            turned[part * width : (part + 1) * width, :] = jnp.transpose(
                z_wide[pl.ds(2 * index + part, edges, stride=2 * len(outs)), :]
            ).astype(BF16)
        for slot in range(slots):
            out[slot] = lax.dot_general(
                turned[...],
                selector[slot * margin : (slot + 1) * margin, :],
                (((1,), (1,)), ((), ())),
                preferred_element_type=F32,
            ).astype(BF16)


def project(sets, width, slots, held):
    _, _, selector, z_wide = held
    margin, edges = selector.shape[0] // slots, selector.shape[1]
    vmem = pl.BlockSpec(memory_space=pltpu.VMEM)
    return pl.pallas_call(
        functools.partial(project_kernel, width),
        out_shape=[pltpu.VMEM((slots, 2 * width, margin), BF16)] * sets,
        in_specs=[vmem] * 2,
        out_specs=[vmem] * sets,
        scratch_shapes=[pltpu.VMEM((2 * width, edges), BF16)],
        compiler_params=pltpu.CompilerParams(vmem_limit_bytes=SMALL_VMEM),
        cost_estimate=pl.CostEstimate(
            flops=4 * edges * width * slots * margin * sets, bytes_accessed=6 << 20, transcendentals=0
        ),
        name="project",
    )(*in_vmem(selector, z_wide))


def gram_kernel(plans, count, group, width, hops, capacity, owners_ref, *rest):
    projectors, rest = rest[: len(group)], rest[len(group) :]
    slots = projectors[0].shape[0]
    incoming, outs, packed = rest[:slots], rest[slots : slots + hops], rest[-1]
    me = lax.axis_index("grp")
    here = lax.axis_index("dom")
    packed[...] = jnp.zeros_like(packed)
    step = 2 * width
    for slot in range(slots):
        mine = exchange_slot(plans[slot], count, here)
        owner = owners_ref[0, mine]
        rank = jnp.int32(0)
        for other in range(slots):
            same = (owners_ref[0, other] == owner) & (other < mine)
            rank += same.astype(jnp.int32)
        place = hop_to(me, owner, hops) * capacity + rank
        for at in range(len(group)):
            gram = jnp.dot(
                projectors[at][slot],
                incoming[slot][:, at * step : (at + 1) * step],
                preferred_element_type=F32,
            )
            packed[place, at, 0] = (gram[:width, :width] - gram[width:, width:]).astype(BF16)
            packed[place, at, 1] = (gram[:width, width:] + gram[width:, :width]).astype(BF16)
    for hop in range(hops):
        outs[hop][...] = packed[hop * capacity : (hop + 1) * capacity]


def gram_blocks(plans, count, group, width, hops, capacity, owners, projectors, incoming):
    smem = pl.BlockSpec(memory_space=pltpu.SMEM)
    vmem = pl.BlockSpec(memory_space=pltpu.VMEM)
    block = (capacity, len(group), 2, width, width)
    slots, _, margin = projectors[0].shape
    return pl.pallas_call(
        functools.partial(gram_kernel, plans, count, group, width, hops, capacity),
        out_shape=[jax.ShapeDtypeStruct(block, BF16)] * hops,
        in_specs=[smem] + [vmem] * (len(group) + len(incoming)),
        out_specs=[vmem] * hops,
        scratch_shapes=[pltpu.VMEM((hops * capacity,) + block[1:], BF16)],
        compiler_params=pltpu.CompilerParams(vmem_limit_bytes=SMALL_VMEM),
        cost_estimate=pl.CostEstimate(
            flops=2 * slots * margin * 4 * width * width * len(group),
            bytes_accessed=2 << 20,
            transcendentals=0,
        ),
    )(owners, *projectors, *incoming)


def spread(group, sets, width, capacity, arrived, held):
    hops = len(arrived)
    vmem = pl.BlockSpec(memory_space=pltpu.VMEM)
    any_space = pl.BlockSpec(memory_space=pl.ANY)
    places = hops * capacity
    extra = [] if held is None else [held]

    def body(*rest):
        inputs, (out_ref, wide, sem) = rest[:hops], rest[-3:]
        mine = lax.axis_index("grp")
        copies = []
        for hop in range(hops):
            source = hop_from(mine, hop, hops)
            for place in range(capacity):
                wide[source * capacity + place] = inputs[hop][place].astype(F32)
            span = pl.ds(source * capacity, capacity)
            copy = pltpu.make_async_copy(
                wide.at[span],
                out_ref.at[span, group[0] : group[0] + len(group)],
                sem.at[hop],
            )
            copy.start()
            copies.append(copy)
        for copy in copies:
            copy.wait()

    return pl.pallas_call(
        body,
        out_shape=jax.ShapeDtypeStruct((places, sets, 2, width, width), F32),
        in_specs=[vmem] * hops + [any_space] * len(extra),
        out_specs=any_space,
        scratch_shapes=[
            pltpu.VMEM((places, len(group), 2, width, width), F32),
            pltpu.SemaphoreType.DMA((hops,)),
        ],
        input_output_aliases={hops: 0} if extra else {},
        compiler_params=pltpu.CompilerParams(vmem_limit_bytes=SMALL_VMEM),
        cost_estimate=pl.CostEstimate(flops=1 << 20, bytes_accessed=2 << 20, transcendentals=0),
    )(*arrived, *extra)


def exchanged(plans, count, outgoing):
    pieces = [None] * len(outgoing)
    for place, (kind, amount) in enumerate(plans):
        if kind == "xor":
            pairs, back = [(node, node ^ amount) for node in range(count)], place
        else:
            pairs = [(node, (node + amount) % count) for node in range(count)]
            back = plans.index((kind, -amount))
        pieces[back] = lax.ppermute(outgoing[place], "dom", pairs)
    return pieces


def on_device(deflation, inverse, operator, neighbours, counts, margin_rows, owners):
    _, edges, sets, _, width = deflation.shape
    _, slots, margin = margin_rows.shape
    group_count = lax.axis_size("grp")
    capacity = (slots + group_count - 1) // group_count
    z = deflation.reshape(edges * sets * 2, width)
    rows = margin_rows.reshape(slots, 1, margin)
    owned = owners.reshape(1, slots)
    count = lax.axis_size("dom")
    plans = exchange_plan(count)
    arrived = []
    for index in range(sets):
        if index == 0:
            outgoing, held, image = first_chain(
                plans, count, sets, width, counts, neighbours, rows, z, inverse[0], operator[0]
            )
        else:
            outgoing = next_chain(index, sets, width, slots, held)
        if index == 0:
            outgoing = list(outgoing) + list(later_pick(slots, width, held, image))
        arrived.append(exchanged(plans, count, outgoing))
    projectors = project(sets, width, slots, held)
    received = []
    for index, pieces in enumerate(arrived):
        blocks = gram_blocks(
            plans, count, (index,), width, group_count, capacity, owned, [projectors[index]], pieces
        )
        sent = [blocks[0]]
        for hop in range(1, group_count):
            pairs = [(s, partner(s, hop, group_count)) for s in range(group_count)]
            sent.append(lax.ppermute(blocks[hop], "grp", pairs))
        received.append(sent)
    result = None
    for index in range(sets):
        result = spread((index,), sets, width, capacity, received[index], result)
    return result


def solution(mesh):
    placed = (
        P(("dom", "grp"), None, None, None, None),
        P(("dom", "grp"), None, None, None),
        P(("dom", "grp"), None, None, None),
        P(("dom", "grp"), None),
        P(("dom", "grp"), None),
        P(("dom", "grp"), None, None),
        P(("dom", "grp"), None, None),
    )
    return jax.shard_map(
        on_device,
        mesh=mesh,
        in_specs=placed,
        out_specs=P(("dom", "grp"), None, None, None, None),
        check_vma=False,
    )
```

```python
import functools

import jax
import jax.numpy as jnp
from jax import lax
from jax.experimental import pallas as pl
from jax.experimental.pallas import tpu as pltpu
from jax.sharding import PartitionSpec as P


OFFSETS = (-3, -2, -1, 1, 2, 3)
F32 = jnp.float32
BF16 = jnp.bfloat16
CHAIN_VMEM = 16 * 1024 * 1024
SMALL_VMEM = 12 * 1024 * 1024


def exchange_plan(count):
    wanted = sorted(offset % count for offset in OFFSETS)
    masks = [
        mask
        for mask in range(1, count)
        if all(((node ^ mask) - node) % count in wanted for node in range(count))
    ]
    if count & (count - 1) == 0 and len(masks) == len(OFFSETS):
        masks.sort(key=lambda mask: (mask < count // 2, bin(mask).count("1"), -mask))
        return [("xor", mask) for mask in masks]
    return [("shift", offset) for offset in OFFSETS[::-1]]


def exchange_slot(plan, count, me):
    kind, amount = plan
    if kind == "shift":
        return OFFSETS.index(amount)
    step = lax.rem((me ^ amount) - me + count, count)
    slot = jnp.int32(0)
    for index, offset in enumerate(OFFSETS):
        slot += jnp.where(step == offset % count, index, 0)
    return slot


def partner(index, hop, count):
    if count & (count - 1) == 0:
        return index ^ hop
    return (index + hop) % count


def hop_to(index, target, count):
    if count & (count - 1) == 0:
        return index ^ target
    return lax.rem(target - index + count, count)


def hop_from(index, hop, count):
    if count & (count - 1) == 0:
        return index ^ hop
    return lax.rem(index - hop + count, count)


def fill_selector(plans, count, rows_ref, counts_ref, neighbours_ref, selector):
    slots, _, margin = rows_ref.shape
    edges = selector.shape[1]
    me = lax.axis_index("dom")
    positions = lax.broadcasted_iota(jnp.int32, (1, margin), 1)
    lanes = lax.broadcasted_iota(jnp.int32, (1, edges), 1).astype(F32)
    masked = []
    for place in range(8):
        if place < slots:
            slot = exchange_slot(plans[place], count, me)
            live = (positions < counts_ref[0, slot]) & (neighbours_ref[0, slot] >= 0)
            masked.append(jnp.where(live, rows_ref[slot], -1).astype(F32))
        else:
            masked.append(jnp.full((1, margin), -1.0, F32))
    columns = jnp.transpose(jnp.concatenate(masked, axis=0))
    for place in range(slots):
        hit = columns[:, place : place + 1] == lanes
        selector[place * margin : (place + 1) * margin, :] = jnp.where(hit, 1.0, 0.0).astype(BF16)


def gather_vectors(z_wide, index, sets, width, a, b):
    edges = a.shape[0]
    real = z_wide[pl.ds(2 * index, edges, stride=2 * sets), :]
    imag = z_wide[pl.ds(2 * index + 1, edges, stride=2 * sets), :]
    a[:, :width] = real.astype(BF16)
    a[:, width:] = imag.astype(BF16)
    b[:, :width] = (-imag).astype(BF16)
    b[:, width:] = real.astype(BF16)


def apply(matrix, waits, width, a, b, to_a, to_b):
    edges = a.shape[0]
    block = edges // 4
    for part in range(4):
        if part in waits:
            waits[part]()
        at = slice(part * block, (part + 1) * block)
        total = jnp.dot(matrix[0, at, :], a[...], preferred_element_type=F32)
        total += jnp.dot(matrix[1, at, :], b[...], preferred_element_type=F32)
        to_a[at, :] = total.astype(BF16)
        if to_b is not None:
            to_b[at, :width] = (-total[:, width:]).astype(BF16)
            to_b[at, width:] = total[:, :width].astype(BF16)


def pick_rows(selector, image, outs):
    margin = outs[0].shape[0]
    for slot, out in enumerate(outs):
        out[...] = jnp.dot(
            selector[slot * margin : (slot + 1) * margin, :], image[...], preferred_element_type=F32
        ).astype(BF16)


def first_chain_kernel(plans, count, sets, width, *refs):
    z_ref, inverse_ref, operator_ref = refs[3:6]
    slots = refs[2].shape[0]
    early = slots // 2
    outs = refs[6 : 6 + early]
    inverse, operator, selector, z_wide, image = refs[6 + early : 11 + early]
    counts, neighbours, rows, z_in, first_a, first_b, second_a, second_b, sems = refs[11 + early :]
    block = inverse.shape[1] // 2

    def fetch(source, target, part, sem):
        at = pl.ds(part * block, block)
        return pltpu.make_async_copy(source.at[:, at], target.at[:, at], sem)

    z_copy = pltpu.make_async_copy(z_ref, z_in, sems.at[0])
    inverse_loads = [fetch(inverse_ref, inverse, part, sems.at[1 + part]) for part in range(2)]
    operator_loads = [fetch(operator_ref, operator, part, sems.at[3 + part]) for part in range(2)]
    small = [
        pltpu.make_async_copy(source, target, sems.at[5 + index])
        for index, (source, target) in enumerate(zip(refs[:3], (counts, neighbours, rows)))
    ]
    for copy in small + [z_copy] + inverse_loads:
        copy.start()
    for copy in small:
        copy.wait()
    fill_selector(plans, count, rows, counts, neighbours, selector)
    z_copy.wait()
    z_wide[...] = z_in[...].astype(F32)
    gather_vectors(z_wide, 0, sets, width, first_a, first_b)

    def begin():
        inverse_loads[0].wait()
        for copy in operator_loads:
            copy.start()

    waits = {2: inverse_loads[1].wait}
    apply(inverse, {0: begin, **waits}, width, first_a, first_b, second_a, second_b)
    apply(inverse, {}, width, second_a, second_b, first_a, first_b)

    def ready():
        operator_loads[0].wait()
        operator_loads[1].wait()

    apply(operator, {0: ready}, width, first_a, first_b, image, None)
    pick_rows(selector, image, outs)


def later_pick(slots, width, held, image):
    _, _, selector, _ = held
    margin = selector.shape[0] // slots
    early = slots // 2
    vmem = pl.BlockSpec(memory_space=pltpu.VMEM)

    def body(selector_ref, image_ref, *outs):
        pick_rows(selector_ref.at[early * margin :], image_ref, outs)

    return pl.pallas_call(
        body,
        out_shape=[pltpu.VMEM((margin, 2 * width), BF16)] * (slots - early),
        in_specs=[vmem] * 2,
        out_specs=[vmem] * (slots - early),
        compiler_params=pltpu.CompilerParams(vmem_limit_bytes=SMALL_VMEM),
        cost_estimate=pl.CostEstimate(
            flops=4 * image.shape[0] * width * slots * margin // 2,
            bytes_accessed=4 << 20,
            transcendentals=0,
        ),
        name="pick0",
    )(*in_vmem(selector, image))


def in_hbm(*values):
    return [pltpu.with_memory_space_constraint(value, pltpu.HBM) for value in values]


def in_vmem(*values):
    return [pltpu.with_memory_space_constraint(value, pltpu.VMEM) for value in values]


def first_chain(plans, count, sets, width, counts, neighbours, rows, z, inverse, operator):
    slots, _, margin = rows.shape
    edges = inverse.shape[1]
    hbm = pl.BlockSpec(memory_space=pltpu.HBM)
    vmem = pl.BlockSpec(memory_space=pltpu.VMEM)
    flops = 4 * edges * width * (6 * edges + slots * margin)
    early = slots // 2
    outs = [pltpu.VMEM((margin, 2 * width), BF16)] * early + [
        pltpu.VMEM(inverse.shape, BF16),
        pltpu.VMEM(operator.shape, BF16),
        pltpu.VMEM((slots * margin, edges), BF16),
        pltpu.VMEM(z.shape, F32),
        pltpu.VMEM((edges, 2 * width), BF16),
    ]
    results = pl.pallas_call(
        functools.partial(first_chain_kernel, plans, count, sets, width),
        out_shape=outs,
        in_specs=[hbm] * 6,
        out_specs=[vmem] * len(outs),
        scratch_shapes=[
            pltpu.SMEM(counts.shape, jnp.int32),
            pltpu.SMEM(neighbours.shape, jnp.int32),
            pltpu.VMEM(rows.shape, jnp.int32),
            pltpu.VMEM(z.shape, BF16),
        ]
        + [pltpu.VMEM((edges, 2 * width), BF16)] * 4
        + [pltpu.SemaphoreType.DMA((8,))],
        compiler_params=pltpu.CompilerParams(vmem_limit_bytes=CHAIN_VMEM),
        cost_estimate=pl.CostEstimate(flops=flops, bytes_accessed=12 << 20, transcendentals=0),
        name="chain0",
    )(*in_hbm(counts, neighbours, rows, z, inverse, operator))
    return results[:early], results[early:-1], results[-1]


def next_chain_kernel(index, sets, width, inverse, operator, selector, z_wide, *refs):
    outs, (first_a, first_b, second_a, second_b) = refs[:-4], refs[-4:]
    gather_vectors(z_wide, index, sets, width, first_a, first_b)
    apply(inverse, {}, width, first_a, first_b, second_a, second_b)
    apply(inverse, {}, width, second_a, second_b, first_a, first_b)
    apply(operator, {}, width, first_a, first_b, second_a, None)
    pick_rows(selector, second_a, outs)


def next_chain(index, sets, width, slots, held):
    inverse, _, selector, _ = held
    edges = inverse.shape[1]
    margin = selector.shape[0] // slots
    vmem = pl.BlockSpec(memory_space=pltpu.VMEM)
    flops = 4 * edges * width * (6 * edges + slots * margin)
    return pl.pallas_call(
        functools.partial(next_chain_kernel, index, sets, width),
        out_shape=[pltpu.VMEM((margin, 2 * width), BF16)] * slots,
        in_specs=[vmem] * 4,
        out_specs=[vmem] * slots,
        scratch_shapes=[pltpu.VMEM((edges, 2 * width), BF16)] * 4,
        compiler_params=pltpu.CompilerParams(vmem_limit_bytes=SMALL_VMEM),
        cost_estimate=pl.CostEstimate(flops=flops, bytes_accessed=12 << 20, transcendentals=0),
    )(*in_vmem(*held))


def project_kernel(width, selector, z_wide, *refs):
    outs, turned = refs[:-1], refs[-1]
    edges = turned.shape[1]
    slots, _, margin = outs[0].shape
    for index, out in enumerate(outs):
        for part in range(2):
            turned[part * width : (part + 1) * width, :] = jnp.transpose(
                z_wide[pl.ds(2 * index + part, edges, stride=2 * len(outs)), :]
            ).astype(BF16)
        for slot in range(slots):
            out[slot] = lax.dot_general(
                turned[...],
                selector[slot * margin : (slot + 1) * margin, :],
                (((1,), (1,)), ((), ())),
                preferred_element_type=F32,
            ).astype(BF16)


def project(sets, width, slots, held):
    _, _, selector, z_wide = held
    margin, edges = selector.shape[0] // slots, selector.shape[1]
    vmem = pl.BlockSpec(memory_space=pltpu.VMEM)
    return pl.pallas_call(
        functools.partial(project_kernel, width),
        out_shape=[pltpu.VMEM((slots, 2 * width, margin), BF16)] * sets,
        in_specs=[vmem] * 2,
        out_specs=[vmem] * sets,
        scratch_shapes=[pltpu.VMEM((2 * width, edges), BF16)],
        compiler_params=pltpu.CompilerParams(vmem_limit_bytes=SMALL_VMEM),
        cost_estimate=pl.CostEstimate(
            flops=4 * edges * width * slots * margin * sets, bytes_accessed=6 << 20, transcendentals=0
        ),
        name="project",
    )(*in_vmem(selector, z_wide))


def gram_kernel(plans, count, group, width, hops, capacity, owners_ref, *rest):
    projectors, rest = rest[: len(group)], rest[len(group) :]
    slots = projectors[0].shape[0]
    incoming, outs, packed = rest[:slots], rest[slots : slots + hops], rest[-1]
    me = lax.axis_index("grp")
    here = lax.axis_index("dom")
    packed[...] = jnp.zeros_like(packed)
    step = 2 * width
    for slot in range(slots):
        mine = exchange_slot(plans[slot], count, here)
        owner = owners_ref[0, mine]
        rank = jnp.int32(0)
        for other in range(slots):
            same = (owners_ref[0, other] == owner) & (other < mine)
            rank += same.astype(jnp.int32)
        place = hop_to(me, owner, hops) * capacity + rank
        for at in range(len(group)):
            gram = jnp.dot(
                projectors[at][slot],
                incoming[slot][:, at * step : (at + 1) * step],
                preferred_element_type=F32,
            )
            packed[place, at, 0] = (gram[:width, :width] - gram[width:, width:]).astype(BF16)
            packed[place, at, 1] = (gram[:width, width:] + gram[width:, :width]).astype(BF16)
    for hop in range(hops):
        outs[hop][...] = packed[hop * capacity : (hop + 1) * capacity]


def gram_blocks(plans, count, group, width, hops, capacity, owners, projectors, incoming):
    smem = pl.BlockSpec(memory_space=pltpu.SMEM)
    vmem = pl.BlockSpec(memory_space=pltpu.VMEM)
    block = (capacity, len(group), 2, width, width)
    slots, _, margin = projectors[0].shape
    return pl.pallas_call(
        functools.partial(gram_kernel, plans, count, group, width, hops, capacity),
        out_shape=[jax.ShapeDtypeStruct(block, BF16)] * hops,
        in_specs=[smem] + [vmem] * (len(group) + len(incoming)),
        out_specs=[vmem] * hops,
        scratch_shapes=[pltpu.VMEM((hops * capacity,) + block[1:], BF16)],
        compiler_params=pltpu.CompilerParams(vmem_limit_bytes=SMALL_VMEM),
        cost_estimate=pl.CostEstimate(
            flops=2 * slots * margin * 4 * width * width * len(group),
            bytes_accessed=2 << 20,
            transcendentals=0,
        ),
    )(owners, *projectors, *incoming)


def spread(group, sets, width, capacity, chosen_hops, received, held):
    total_hops = len(received)
    arrived = [received[hop] for hop in chosen_hops]
    hops = len(arrived)
    vmem = pl.BlockSpec(memory_space=pltpu.VMEM)
    any_space = pl.BlockSpec(memory_space=pl.ANY)
    places = total_hops * capacity
    extra = [] if held is None else [held]

    def body(*rest):
        inputs, (out_ref, wide, sem) = rest[:hops], rest[-3:]
        mine = lax.axis_index("grp")
        copies = []
        for hop in range(hops):
            source = hop_from(mine, chosen_hops[hop], total_hops)
            wide[hop * capacity : (hop + 1) * capacity] = inputs[hop][...].astype(F32)
            span = pl.ds(source * capacity, capacity)
            copy = pltpu.make_async_copy(
                wide.at[pl.ds(hop * capacity, capacity)],
                out_ref.at[span, group[0] : group[0] + len(group)],
                sem.at[hop],
            )
            copy.start()
            copies.append(copy)
        for copy in copies:
            copy.wait()

    return pl.pallas_call(
        body,
        out_shape=jax.ShapeDtypeStruct((places, sets, 2, width, width), F32),
        in_specs=[vmem] * hops + [any_space] * len(extra),
        out_specs=any_space,
        scratch_shapes=[
            pltpu.VMEM((hops * capacity, len(group), 2, width, width), F32),
            pltpu.SemaphoreType.DMA((hops,)),
        ],
        input_output_aliases={hops: 0} if extra else {},
        compiler_params=pltpu.CompilerParams(vmem_limit_bytes=SMALL_VMEM),
        cost_estimate=pl.CostEstimate(flops=1 << 20, bytes_accessed=2 << 20, transcendentals=0),
    )(*arrived, *extra)


def exchanged(plans, count, outgoing):
    pieces = [None] * len(outgoing)
    for place, (kind, amount) in enumerate(plans):
        if kind == "xor":
            pairs, back = [(node, node ^ amount) for node in range(count)], place
        else:
            pairs = [(node, (node + amount) % count) for node in range(count)]
            back = plans.index((kind, -amount))
        pieces[back] = lax.ppermute(outgoing[place], "dom", pairs)
    return pieces


def on_device(deflation, inverse, operator, neighbours, counts, margin_rows, owners):
    _, edges, sets, _, width = deflation.shape
    _, slots, margin = margin_rows.shape
    group_count = lax.axis_size("grp")
    capacity = (slots + group_count - 1) // group_count
    z = deflation.reshape(edges * sets * 2, width)
    rows = margin_rows.reshape(slots, 1, margin)
    owned = owners.reshape(1, slots)
    count = lax.axis_size("dom")
    plans = exchange_plan(count)
    arrived = []
    for index in range(sets):
        if index == 0:
            outgoing, held, image = first_chain(
                plans, count, sets, width, counts, neighbours, rows, z, inverse[0], operator[0]
            )
        else:
            outgoing = next_chain(index, sets, width, slots, held)
        if index == 0:
            outgoing = list(outgoing) + list(later_pick(slots, width, held, image))
        arrived.append(exchanged(plans, count, outgoing))
    projectors = project(sets, width, slots, held)
    received = []
    for index, pieces in enumerate(arrived):
        blocks = gram_blocks(
            plans, count, (index,), width, group_count, capacity, owned, [projectors[index]], pieces
        )
        sent = [blocks[0]]
        for hop in range(1, group_count):
            pairs = [(s, partner(s, hop, group_count)) for s in range(group_count)]
            sent.append(lax.ppermute(blocks[hop], "grp", pairs))
        received.append(sent)
    result = None
    everyone = tuple(range(group_count))
    for index in range(sets - 1):
        result = spread((index,), sets, width, capacity, everyone, received[index], result)
    index, near = sets - 1, everyone[: group_count // 2]
    for hops in (near, everyone[len(near) :]):
        result = spread((index,), sets, width, capacity, hops, received[index], result)
    return result


def solution(mesh):
    placed = (
        P(("dom", "grp"), None, None, None, None),
        P(("dom", "grp"), None, None, None),
        P(("dom", "grp"), None, None, None),
        P(("dom", "grp"), None),
        P(("dom", "grp"), None),
        P(("dom", "grp"), None, None),
        P(("dom", "grp"), None, None),
    )
    return jax.shard_map(
        on_device,
        mesh=mesh,
        in_specs=placed,
        out_specs=P(("dom", "grp"), None, None, None, None),
        check_vma=False,
    )
```
